32 devices in a mesh: data: 1 (over z), dap: 32 (over y, x, core).
Axes of the slice: x: 4, y: 4, z: 1, core: 2. Of those that a mesh axis runs over, the one named last changes fastest.
The devices are a block of a 4x4x8 slice.
Arguments:
- z_one: bfloat16 [768, 768, 128], P(('data', 'dap'))
- mask_one: int32 [768, 768], P(('data', 'dap'))
- z_two: bfloat16 [768, 768, 128], P(('data', 'dap'))
- mask_two: int32 [768, 768], P(('data', 'dap'))
- norm_in: bfloat16 [2, 2, 128], replicated
- w_proj: bfloat16 [2, 128, 512], replicated
- w_gate: bfloat16 [2, 128, 128], replicated
- norm_mid: bfloat16 [2, 2, 128], replicated
- w_out: bfloat16 [2, 128, 128], replicated
Outputs:
- output 1: bfloat16 [768, 768, 128], P(('data', 'dap'))
- output 2: bfloat16 [768, 768, 128], P(('data', 'dap'))
All inputs are finite; a program needn't handle non-finite values.
Results may differ from the reference program's by a relative error of at most 0.00449604.
Values are sent between devices in bfloat16 or wider.
A program may use at most 768 MiB of HBM per device.

```python
import jax
import jax.numpy as jnp
from jax import lax

N = 768
CZ = 128
C = 128


def layer_norm(vals, ln_gain, ln_shift):
    vals = vals.astype(jnp.float32)
    row_mean = jnp.mean(vals, axis=-1, keepdims=True)
    centred = vals - row_mean
    row_var = jnp.mean(centred * centred, axis=-1, keepdims=True)
    return centred * lax.rsqrt(row_var + 1e-5) * ln_gain.astype(jnp.float32) + ln_shift.astype(jnp.float32)


def draw_mask(mask_key):
    residue_ok = (jax.random.randint(mask_key, (N,), 0, 20) != 0).astype(jnp.int32)
    return residue_ok[:, None] * residue_ok[None, :]


def setup_inputs(seed: int = 0, part: int = 0) -> dict:
    part_keys = jax.random.split(jax.random.fold_in(jax.random.key(seed), part), 4)
    shared_keys = jax.random.split(jax.random.key(seed + 1), 5)
    norm_base = jnp.array([1.0, 0.0], jnp.float32)[None, :, None]
    return {
        "z_one": jax.random.normal(part_keys[0], (N, N, CZ), jnp.float32).astype(jnp.bfloat16),
        "mask_one": draw_mask(part_keys[1]),
        "z_two": jax.random.normal(part_keys[2], (N, N, CZ), jnp.float32).astype(jnp.bfloat16),
        "mask_two": draw_mask(part_keys[3]),
        "norm_in": (0.3 * jax.random.normal(shared_keys[0], (2, 2, CZ), jnp.float32) + norm_base).astype(jnp.bfloat16),
        "w_proj": (jax.random.normal(shared_keys[1], (2, CZ, 4 * C), jnp.float32) * CZ ** -0.5).astype(jnp.bfloat16),
        "w_gate": (jax.random.normal(shared_keys[2], (2, CZ, CZ), jnp.float32) * CZ ** -0.5).astype(jnp.bfloat16),
        "norm_mid": (0.3 * jax.random.normal(shared_keys[3], (2, 2, C), jnp.float32) + norm_base).astype(jnp.bfloat16),
        "w_out": (jax.random.normal(shared_keys[4], (2, C, CZ), jnp.float32) * C ** -0.5).astype(jnp.bfloat16),
    }


def project_row(z_row, mask_row, norm_in, w_proj):
    x_row = layer_norm(z_row, norm_in[0], norm_in[1]).astype(jnp.bfloat16)
    projected = jnp.dot(x_row, w_proj, preferred_element_type=jnp.float32)
    keep_mask = mask_row.astype(jnp.float32)[:, None]
    a_row = keep_mask * jax.nn.sigmoid(projected[:, C:2 * C]) * projected[:, :C]
    b_row = keep_mask * jax.nn.sigmoid(projected[:, 3 * C:]) * projected[:, 2 * C:3 * C]
    return a_row.astype(jnp.bfloat16), b_row.astype(jnp.bfloat16)


def output_row(z_row, t_row, norm_in, w_gate, norm_mid, w_out):
    x_row = layer_norm(z_row, norm_in[0], norm_in[1]).astype(jnp.bfloat16)
    gate_val = jax.nn.sigmoid(jnp.dot(x_row, w_gate, preferred_element_type=jnp.float32))
    t_norm = layer_norm(t_row, norm_mid[0], norm_mid[1]).astype(jnp.bfloat16)
    update = jnp.dot(t_norm, w_out, preferred_element_type=jnp.float32)
    return (z_row.astype(jnp.float32) + gate_val * update).astype(jnp.bfloat16)


def tri_update(z_pair, pair_mask, norm_in, w_proj, w_gate, norm_mid, w_out, form):
    a_side, b_side = lax.map(lambda row_pair: project_row(row_pair[0], row_pair[1], norm_in, w_proj), (z_pair, pair_mask))
    tri_prod = jnp.einsum(form, a_side.astype(jnp.float32), b_side.astype(jnp.float32)).astype(jnp.bfloat16)
    return lax.map(lambda row_pair: output_row(row_pair[0], row_pair[1], norm_in, w_gate, norm_mid, w_out), (z_pair, tri_prod))


def run_crop(z_pair, pair_mask, norm_in, w_proj, w_gate, norm_mid, w_out):
    z_mid = tri_update(z_pair, pair_mask, norm_in[0], w_proj[0], w_gate[0], norm_mid[0], w_out[0], "ikc,jkc->ijc")
    return tri_update(z_mid, pair_mask, norm_in[1], w_proj[1], w_gate[1], norm_mid[1], w_out[1], "kic,kjc->ijc")


def reference(z_one, mask_one, z_two, mask_two, norm_in, w_proj, w_gate, norm_mid, w_out):
    return (run_crop(z_one, mask_one, norm_in, w_proj, w_gate, norm_mid, w_out),
            run_crop(z_two, mask_two, norm_in, w_proj, w_gate, norm_mid, w_out))
```

```python
import functools

import jax
import jax.numpy as jnp
from jax import lax
from jax.experimental import pallas as pl
from jax.experimental.pallas import tpu as pltpu
from jax.sharding import PartitionSpec as P

RB = 8
LANES = 128
F32, BF16 = jnp.float32, jnp.bfloat16


def _norm_cols(v, gain, shift):
    mean = jnp.mean(v, axis=0, keepdims=True)
    cen = v - mean
    var = jnp.mean(cen * cen, axis=0, keepdims=True)
    return (cen * lax.rsqrt(var + 1e-5) * gain + shift).astype(BF16)


def _mm(a, b):
    return lax.dot_general(a, b, (((1,), (0,)), ((), ())), preferred_element_type=F32)


def _project(z_t, norm_ref, wp_ref, scr, r, kk):
    hid = wp_ref.shape[0] // 4
    x_t = _norm_cols(z_t, norm_ref[0], norm_ref[1])
    q = _mm(wp_ref[...], x_t)
    for s in range(2):
        p, g = q[2 * s * hid:(2 * s + 1) * hid], q[(2 * s + 1) * hid:(2 * s + 2) * hid]
        scr[kk, pl.ds(s * hid * RB + r, hid, stride=RB), :] = jax.nn.sigmoid(g) * p


def _emit_sides(scr, m_ref, out_ref, kk):
    n, _, cl = out_ref.shape[:3]
    half = n * cl * RB
    lanes = slice(kk * LANES, (kk + 1) * LANES)
    keep = m_ref[:, lanes].astype(F32)
    for s in range(2):
        for d in range(n):
            v = scr[kk, pl.ds(s * half + d * cl * RB, cl * RB), :].reshape(cl, RB, LANES)
            out_ref[d, s, :, :, lanes] = (v * keep).astype(BF16)


def _finish(z_t, r, kk, scr_y, norm_ref, mid_ref, wg_ref, wo_ref):
    hid = wo_ref.shape[1]
    x_t = _norm_cols(z_t, norm_ref[0], norm_ref[1])
    gate = jax.nn.sigmoid(_mm(wg_ref[...], x_t))
    y = scr_y[kk, pl.ds(r, hid, stride=RB), :]
    y = (y * mid_ref[0] + mid_ref[1]).astype(BF16)
    return (z_t + gate * _mm(wo_ref[...], y)).astype(BF16)


def _norm_mid(t_ref, scr_y, kk):
    n, cl = t_ref.shape[:2]
    lanes = slice(kk * LANES, (kk + 1) * LANES)
    tot = n * cl

    def load(i):
        return t_ref[i, :, :, lanes].astype(F32)

    zero = jnp.zeros((RB, LANES), F32)
    mean = lax.fori_loop(0, n, lambda i, a: a + jnp.sum(load(i), axis=0), zero, unroll=8) * (1.0 / tot)

    def sq(i, a):
        c = load(i) - mean
        return a + jnp.sum(c * c, axis=0)
    var = lax.fori_loop(0, n, sq, zero, unroll=8) * (1.0 / tot)
    inv = lax.rsqrt(var + 1e-5)

    def put(i, c):
        v = (load(i) - mean) * inv
        scr_y[kk, pl.ds(pl.multiple_of(i * cl * RB, cl * RB), cl * RB), :] = v.reshape(cl * RB, LANES)
        return c
    lax.fori_loop(0, n, put, 0, unroll=8)


def _row_loop(f):
    def body(r, c):
        f(r)
        return c
    lax.fori_loop(0, RB, body, 0)


def _project_kernel(z_ref, m_ref, norm_ref, wp_ref, out_ref, scr):
    for kk in range(z_ref.shape[1] // LANES):
        lanes = slice(kk * LANES, (kk + 1) * LANES)

        def row(r):
            z_t = z_ref[r, lanes, :].astype(F32).T
            _project(z_t, norm_ref, wp_ref, scr, r, kk)
        _row_loop(row)
        _emit_sides(scr, m_ref, out_ref, kk)


def _finish_project_kernel(z_ref, t_ref, m_ref, n0_ref, mid_ref, wg_ref, wo_ref, n1_ref, wp_ref, zt_ref, out_ref, scr_y, scr):
    for kk in range(z_ref.shape[1] // LANES):
        lanes = slice(kk * LANES, (kk + 1) * LANES)
        _norm_mid(t_ref, scr_y, kk)

        def row(r):
            z_t = z_ref[r, lanes, :].astype(F32).T
            z_new = _finish(z_t, r, kk, scr_y, n0_ref, mid_ref, wg_ref, wo_ref)
            zt_ref[r, :, lanes] = z_new
            _project(z_new.astype(F32), n1_ref, wp_ref, scr, r, kk)
        _row_loop(row)
        _emit_sides(scr, m_ref, out_ref, kk)


def _finish_kernel(zt_ref, t_ref, n0_ref, mid_ref, wg_ref, wo_ref, z_ref, scr_y):
    for kk in range(z_ref.shape[1] // LANES):
        lanes = slice(kk * LANES, (kk + 1) * LANES)
        _norm_mid(t_ref, scr_y, kk)

        def row(r):
            z_new = _finish(zt_ref[r, :, lanes].astype(F32), r, kk, scr_y, n0_ref, mid_ref, wg_ref, wo_ref)
            z_ref[r, lanes, :] = z_new.astype(F32).T.astype(BF16)
        _row_loop(row)


def _triangle_kernel(contract, a_ref, b_ref, out_ref):
    n, _, _, rows, width = a_ref.shape
    a = a_ref[...].reshape(n * rows, width)
    b = b_ref[...].reshape(n * rows, width)
    t = lax.dot_general(a, b, (((contract,), (contract,)), ((), ())), preferred_element_type=F32)
    out_ref[...] = t.astype(BF16).reshape(out_ref.shape)


def _whole(a):
    return pl.BlockSpec(a.shape, lambda *_: (0,) * a.ndim)


def _cost(flops, nbytes):
    return pl.CostEstimate(flops=flops, bytes_accessed=nbytes, transcendentals=0)


PARAMS = pltpu.CompilerParams(vmem_limit_bytes=60 * 1024 * 1024)


class Shapes:
    def __init__(self, n, z, w_proj):
        self.n, (self.rows, self.width, self.cz) = n, z.shape
        self.hid = w_proj.shape[-1] // 4
        self.cl = self.hid // n
        self.kb = 2 * LANES if self.width % (2 * LANES) == 0 else LANES
        self.grid = (self.rows // RB, self.width // self.kb)
        self.z_spec = pl.BlockSpec((RB, self.kb, self.cz), lambda i, j: (i, j, 0))
        self.zt_spec = pl.BlockSpec((RB, self.cz, self.kb), lambda i, j: (i, 0, j))
        self.m_spec = pl.BlockSpec((RB, self.kb), lambda i, j: (i, j))
        self.sides_spec = pl.BlockSpec((n, 2, self.cl, RB, self.kb), lambda i, j: (0, 0, 0, i, j))
        self.t_spec = pl.BlockSpec((n, self.cl, RB, self.kb), lambda i, j: (0, 0, i, j))
        self.sides = jax.ShapeDtypeStruct((n, 2, self.cl, self.rows, self.width), BF16)
        self.tri = jax.ShapeDtypeStruct((n, self.cl, self.rows, self.width), BF16)
        self.zt = jax.ShapeDtypeStruct((self.rows, self.cz, self.width), BF16)
        self.scr = pltpu.VMEM((self.kb // LANES, 2 * self.hid * RB, LANES), F32)
        self.scr_y = pltpu.VMEM((self.kb // LANES, self.hid * RB, LANES), F32)
        pos = self.rows * self.width
        self.f_proj = 2 * pos * self.cz * 4 * self.hid
        self.f_fin = 4 * pos * self.cz * self.hid
        self.f_tri = 2 * self.cl * self.width ** 3
        self.bytes = 2 * pos * self.cz * 4


def project(sh, z, m, norm, wp):
    return pl.pallas_call(
        _project_kernel, grid=sh.grid, out_shape=sh.sides,
        in_specs=[sh.z_spec, sh.m_spec, _whole(norm), _whole(wp)], out_specs=sh.sides_spec,
        scratch_shapes=[sh.scr], compiler_params=PARAMS, cost_estimate=_cost(sh.f_proj * 8, sh.bytes), name="project",
    )(z, m, norm, wp)


def finish_project(sh, z, t, m, n0, mid, wg, wo, n1, wp):
    return pl.pallas_call(
        _finish_project_kernel, grid=sh.grid, out_shape=(sh.zt, sh.sides),
        in_specs=[sh.z_spec, sh.t_spec, sh.m_spec] + [_whole(a) for a in (n0, mid, wg, wo, n1, wp)],
        out_specs=(sh.zt_spec, sh.sides_spec), scratch_shapes=[sh.scr_y, sh.scr], compiler_params=PARAMS,
        cost_estimate=_cost((sh.f_proj + sh.f_fin) * 8, 2 * sh.bytes), name="finish_project",
    )(z, t, m, n0, mid, wg, wo, n1, wp)


def finish(sh, zt, t, n0, mid, wg, wo):
    return pl.pallas_call(
        _finish_kernel, grid=sh.grid, out_shape=jax.ShapeDtypeStruct((sh.rows, sh.width, sh.cz), BF16),
        in_specs=[sh.zt_spec, sh.t_spec] + [_whole(a) for a in (n0, mid, wg, wo)],
        out_specs=sh.z_spec, scratch_shapes=[sh.scr_y], compiler_params=PARAMS,
        cost_estimate=_cost(sh.f_fin * 8, sh.bytes), name="finish",
    )(zt, t, n0, mid, wg, wo)


def triangle(sh, sides, contract):
    side = lambda s: pl.BlockSpec((sh.n, 1, 1, sh.rows, sh.width), lambda c: (0, s, c, 0, 0))
    return pl.pallas_call(
        functools.partial(_triangle_kernel, contract), grid=(sh.cl,), out_shape=sh.tri,
        in_specs=[side(0), side(1)], out_specs=pl.BlockSpec((sh.n, 1, sh.rows, sh.width), lambda c: (0, c, 0, 0)),
        compiler_params=PARAMS, cost_estimate=_cost(sh.f_tri * 8, sh.bytes), name="triangle",
    )(sides, sides)


def exchange(v):
    return lax.all_to_all(v, "dap", 0, 0, tiled=True)


def _lanes(norm):
    return jnp.broadcast_to(norm.astype(F32)[..., None], norm.shape + (LANES,))


def solution(mesh):
    n = mesh.shape["dap"]
    row_spec = P(("data", "dap"), None, None)
    mask_spec = P(("data", "dap"), None)
    rep = P()

    def per_device(z_one, mask_one, z_two, mask_two, norm_in, w_proj, w_gate, norm_mid, w_out):
        sh = Shapes(n, z_one, w_proj)
        nin, mid = _lanes(norm_in), _lanes(norm_mid)
        wp, wg, wo = (jnp.swapaxes(w, 1, 2) for w in (w_proj, w_gate, w_out))
        zs, ms = (z_one, z_two), (mask_one, mask_two)
        sides = [project(sh, z, m, nin[0], wp[0]) for z, m in zip(zs, ms)]
        got = [exchange(s) for s in sides]
        tri = [exchange(triangle(sh, g, 1)) for g in got]
        mids = [finish_project(sh, z, t, m, nin[0], mid[0], wg[0], wo[0], nin[1], wp[1]) for z, t, m in zip(zs, tri, ms)]
        got = [exchange(s) for _, s in mids]
        tri = [exchange(triangle(sh, g, 0)) for g in got]
        return tuple(finish(sh, zt, t, nin[1], mid[1], wg[1], wo[1]) for (zt, _), t in zip(mids, tri))

    return jax.shard_map(per_device, mesh=mesh,
                         in_specs=(row_spec, mask_spec, row_spec, mask_spec, rep, rep, rep, rep, rep),
                         out_specs=(row_spec, row_spec), check_vma=False)
```

```python
import functools
import math

import jax
import jax.numpy as jnp
from jax import lax
from jax.experimental import pallas as pl
from jax.experimental.pallas import tpu as pltpu
from jax.sharding import PartitionSpec as P

RB = 8
LANES = 128
UNROLL = 4
F32, BF16 = jnp.float32, jnp.bfloat16


def _norm_cols(v, gain, shift):
    mean = jnp.mean(v, axis=0, keepdims=True)
    cen = v - mean
    var = jnp.mean(cen * cen, axis=0, keepdims=True)
    return (cen * lax.rsqrt(var + 1e-5) * gain + shift).astype(BF16)


def _mm(a, b):
    return lax.dot_general(a, b, (((1,), (0,)), ((), ())), preferred_element_type=F32)


def _project(z_t, norm_ref, wp_ref, scr, r, kk):
    hid = wp_ref.shape[0] // 4
    x_t = _norm_cols(z_t, norm_ref[0], norm_ref[1])
    q = _mm(wp_ref[...], x_t)
    for s in range(2):
        p, g = q[2 * s * hid:(2 * s + 1) * hid], q[(2 * s + 1) * hid:(2 * s + 2) * hid]
        scr[kk, pl.ds(s * hid * RB + r, hid, stride=RB), :] = jax.nn.sigmoid(g) * p


def _emit_sides(scr, m_ref, out_ref, kk, topo):
    half = scr.shape[1] // 2
    lanes = slice(kk * LANES, (kk + 1) * LANES)
    keep = m_ref[:, lanes].astype(F32)
    for q in range(topo.nq):
        for rho, owner in topo.blocks(q):
            for s in range(2):
                at = pl.multiple_of(s * half + (owner * topo.nq + q) * RB, RB)
                out_ref[(q, s) + rho + (slice(None), lanes)] = (scr[kk, pl.ds(at, RB), :] * keep).astype(BF16)


def _finish(z_t, r, kk, scr_y, norm_ref, mid_ref, wg_ref, wo_ref):
    hid = wo_ref.shape[1]
    x_t = _norm_cols(z_t, norm_ref[0], norm_ref[1])
    gate = jax.nn.sigmoid(_mm(wg_ref[...], x_t))
    y = scr_y[kk, pl.ds(r, hid, stride=RB), :]
    y = (y * mid_ref[0] + mid_ref[1]).astype(BF16)
    return (z_t + gate * _mm(wo_ref[...], y)).astype(BF16)


def _norm_mid(t_refs, scr_y, kk, topo):
    lanes = slice(kk * LANES, (kk + 1) * LANES)
    tiles = [(q,) + rest for q in range(topo.nq) for rest in topo.landed(q)]
    inv_n = 1.0 / len(tiles)

    def load(tile):
        return t_refs[tile[1]][(tile[0],) + tile[2] + (slice(None), lanes)].astype(F32)

    def total(f):
        part = [f(load(t)) for t in tiles[:4]]
        for i, t in enumerate(tiles[4:]):
            part[i % 4] = part[i % 4] + f(load(t))
        return (part[0] + part[1]) + (part[2] + part[3])
    mean = total(lambda v: v) * inv_n
    inv = lax.rsqrt(total(lambda v: (v - mean) * (v - mean)) * inv_n + 1e-5)
    for t in tiles:
        at = pl.multiple_of((t[3] * topo.nq + t[0]) * RB, RB)
        scr_y[kk, pl.ds(at, RB), :] = (load(t) - mean) * inv


def _row_loop(width, f):
    def body(i, c):
        for u in range(UNROLL):
            for kk in range(width // LANES):
                f(i * UNROLL + u, kk, slice(kk * LANES, (kk + 1) * LANES))
        return c
    lax.fori_loop(0, RB // UNROLL, body, 0)


class Topo:
    def __init__(self, n):
        self.side = math.isqrt(n // 2)
        ring = self.side.bit_length() - 1
        self.nq = 2 * ring
        self.nb = self.nq + 1
        links = [(axis, bit) for bit in range(ring) for axis in ("x", "y")]
        self.order = [[("core", 0)] + [links[(q + i) % self.nq] for i in range(self.nq)] for q in range(self.nq)]
        self.weight = {("core", 0): 1}
        self.weight.update({("x", b): 2 << b for b in range(ring)})
        self.weight.update({("y", b): (2 << ring) << b for b in range(ring)})

    def here(self):
        me = lax.axis_index("dap")
        self.pos = {"core": lax.rem(me, 2), "x": lax.rem(me // 2, self.side), "y": me // (2 * self.side)}
        self.bit = {}
        for axis, b in self.weight:
            v = self.pos[axis]
            self.bit[axis, b] = lax.rem(v // (1 << b) + v // (2 << b), 2) if axis != "core" else v
        return self

    def partner(self, link):
        axis, b = link
        pos = dict(self.pos)
        v, span = pos[axis], 2 << b
        base = v - lax.rem(v, span)
        pos[axis] = base + (span - 1) - lax.rem(v, span)
        return (pos["y"] * self.side + pos["x"]) * 2 + pos["core"]

    def blocks(self, q):
        out = [((), 0)]
        for link in self.order[q]:
            w, own = self.weight[link], self.bit[link]
            out = [(r + (f,), o + w * (1 - own if f else own)) for r, o in out for f in (0, 1)]
        return out

    def landed(self, q):
        out = []
        for rho, owner in self.blocks(q):
            last = max([i for i, f in enumerate(rho) if f], default=-1)
            idx = (0,) * self.nb if last < 0 else rho[:last] + (0,) * (self.nb - last)
            out.append((last + 1, idx, owner))
        return out

    def natural(self, owner):
        side, core, rest = self.side, lax.rem(owner, 2), owner // 2
        gx, gy = lax.rem(rest, side), rest // side

        def binary(g):
            v, b = 0, 0
            k = side.bit_length() - 2
            for i in range(k, -1, -1):
                b = lax.rem(b + lax.rem(g // (1 << i), 2), 2)
                v = v + b * (1 << i)
            return v
        return (binary(gy) * side + binary(gx)) * 2 + core

    def gray_bits(self, p):
        pos = {"core": p % 2, "x": p // 2 % self.side, "y": p // 2 // self.side}
        return {k: (pos[k[0]] if k[0] == "core" else (pos[k[0]] >> k[1] ^ pos[k[0]] >> (k[1] + 1)) & 1) for k in self.weight}

    def relative(self, q, p):
        bits = self.gray_bits(p)
        return tuple((1 - self.bit[k]) if bits[k] else self.bit[k] for k in self.order[q])


class Exchange:
    def __init__(self, topo, src, dst, ssem, rsem):
        self.topo, self.src, self.dst, self.ssem, self.rsem = topo, src, dst, ssem, rsem
        self.cut = src.shape[1] == 1

    def _tail(self, sub):
        if not self.cut:
            return sub, ()
        w = self.src.shape[-1] // 2
        return 0, (slice(None), pl.ds(sub * w, w))

    def _copy(self, q, sub, s, a, b):
        return pltpu.make_async_remote_copy(
            src_ref=a, dst_ref=b, send_sem=self.ssem.at[q, sub, s], recv_sem=self.rsem.at[q, sub, s],
            device_id={"dap": self.topo.partner(self.topo.order[q][s])}, device_id_type=pl.DeviceIdType.MESH)

    def start(self, sub, s):
        nb, free = self.topo.nb, (slice(None),)
        k, tail = self._tail(sub)
        for q in range(self.topo.nq):
            for t in range(-1, s):
                if t < 0:
                    idx = (0,) * s + (1,) + free * (nb - 1 - s) + tail
                    a = self.src.at[(q, k) + idx]
                else:
                    idx = free * t + (1,) + (0,) * (s - 1 - t) + (1,) + free * (nb - 1 - s) + tail
                    a = self.dst.at[(q, k, t) + idx]
                self._copy(q, sub, s, a, self.dst.at[(q, k, s) + idx]).start()

    def _whole(self, q, sub, s):
        k, tail = self._tail(sub)
        ref = self.dst.at[(q, k, s) + (slice(None),) * s + (1,) + (slice(None),) * (self.topo.nb - 1 - s) + tail]
        return self._copy(q, sub, s, ref, ref)

    def arrive(self, sub, s):
        for q in range(self.topo.nq):
            self._whole(q, sub, s).wait_recv()

    def drain(self):
        for sub in range(2):
            for s in range(self.topo.nb):
                for q in range(self.topo.nq):
                    self._whole(q, sub, s).wait_send()

    def barrier(self):
        bar = pltpu.get_barrier_semaphore()
        for link in self.topo.weight:
            pl.semaphore_signal(bar, inc=1, device_id={"dap": self.topo.partner(link)}, device_id_type=pl.DeviceIdType.MESH)
        pl.semaphore_wait(bar, len(self.topo.weight))

    def moves(self):
        out = []
        for s in range(self.topo.nb):
            for sub in range(2):
                def move(s=s, sub=sub):
                    self.arrive(sub, s)
                    if s + 1 < self.topo.nb:
                        self.start(sub, s + 1)
                out.append(move)
        return out


def _project_kernel(topo, z_ref, m_ref, norm_ref, wp_ref, out_ref, scr):
    def row(r, kk, lanes):
        _project(z_ref[r, lanes, :].astype(F32).T, norm_ref, wp_ref, scr, r, kk)
    _row_loop(z_ref.shape[1], row)
    for kk in range(z_ref.shape[1] // LANES):
        _emit_sides(scr, m_ref, out_ref, kk, topo)


def _finish_project_kernel(topo, z_ref, m_ref, n0_ref, mid_ref, wg_ref, wo_ref, n1_ref, wp_ref, *refs):
    t_refs, (zt_ref, out_ref, scr_y, scr) = refs[:-4], refs[-4:]
    for kk in range(z_ref.shape[1] // LANES):
        _norm_mid(t_refs, scr_y, kk, topo)

    def row(r, kk, lanes):
        z_t = z_ref[r, lanes, :].astype(F32).T
        z_new = _finish(z_t, r, kk, scr_y, n0_ref, mid_ref, wg_ref, wo_ref)
        zt_ref[r, :, lanes] = z_new
        _project(z_new.astype(F32), n1_ref, wp_ref, scr, r, kk)
    _row_loop(z_ref.shape[1], row)
    for kk in range(z_ref.shape[1] // LANES):
        _emit_sides(scr, m_ref, out_ref, kk, topo)


def _finish_kernel(topo, zt_ref, n0_ref, mid_ref, wg_ref, wo_ref, *refs):
    t_refs, (z_ref, scr_y) = refs[:-2], refs[-2:]
    for kk in range(z_ref.shape[1] // LANES):
        _norm_mid(t_refs, scr_y, kk, topo)

    def row(r, kk, lanes):
        z_new = _finish(zt_ref[r, :, lanes].astype(F32), r, kk, scr_y, n0_ref, mid_ref, wg_ref, wo_ref)
        z_ref[r, lanes, :] = z_new.astype(F32).T.astype(BF16)
    _row_loop(z_ref.shape[1], row)


def _triangle_kernel(topo, contract, *refs):
    half = (len(refs) - 3) // 2
    a_refs, b_refs, (out_ref, a_scr, b_scr) = refs[:half], refs[half:2 * half], refs[-3:]
    n, rows, width = a_scr.shape
    step = pl.program_id(0)

    def gather(q):
        for i, (piece, idx, owner) in enumerate(topo.landed(q)):
            a_scr[i] = a_refs[piece][(0,) + idx]
            b_scr[topo.natural(owner) if contract else i] = b_refs[piece][(0,) + idx]

    def scatter(q):
        for p in range(n):
            out_ref[(0,) + topo.relative(q, p)] = a_scr[p]
    for q in range(topo.nq):
        pl.when(step == q)(functools.partial(gather, q))
    a, b = a_scr[...].reshape(n * rows, width), b_scr[...].reshape(n * rows, width)
    t = lax.dot_general(a, b, (((contract,), (contract,)), ((), ())), preferred_element_type=F32)
    t = t.astype(BF16).reshape(n, rows, width)
    if contract:
        out_ref[...] = t.reshape(out_ref.shape)
    else:
        a_scr[...] = t
        for q in range(topo.nq):
            pl.when(step == q)(functools.partial(scatter, q))


def _whole(a):
    return pl.BlockSpec(a.shape, lambda *_: (0,) * a.ndim)


class Shapes:
    def __init__(self, n, z, w_proj):
        self.topo = topo = Topo(n)
        self.n, (self.rows, self.width, self.cz) = n, z.shape
        self.hid = w_proj.shape[-1] // 4
        assert self.hid == n * topo.nq
        self.kb = 2 * LANES if self.width % (2 * LANES) == 0 else LANES
        self.grid = (self.rows // RB, self.width // self.kb)
        self.bits = (2,) * topo.nb
        zero = (0,) * topo.nb
        self.z_spec = pl.BlockSpec((RB, self.kb, self.cz), lambda i, j: (i, j, 0))
        self.zt_spec = pl.BlockSpec((RB, self.cz, self.kb), lambda i, j: (i, 0, j))
        self.m_spec = pl.BlockSpec((RB, self.kb), lambda i, j: (i, j))
        self.sides_spec = pl.BlockSpec((topo.nq, 2) + self.bits + (RB, self.kb), lambda i, j: (0, 0) + zero + (i, j))
        self.sides = jax.ShapeDtypeStruct((topo.nq, 2) + self.bits + (self.rows, self.width), BF16)
        self.tri = jax.ShapeDtypeStruct((topo.nq, 1) + self.bits + (self.rows, self.width), BF16)
        self.zt = jax.ShapeDtypeStruct((self.rows, self.cz, self.width), BF16)
        self.scr = pltpu.VMEM((self.kb // LANES, 2 * self.hid * RB, LANES), F32)
        self.scr_y = pltpu.VMEM((self.kb // LANES, self.hid * RB, LANES), F32)
        self.mat = pltpu.VMEM((n, self.rows, self.width), BF16)

    def landing(self, src):
        return jax.ShapeDtypeStruct(src.shape[:2] + (self.topo.nb,) + src.shape[2:], BF16)

    def _pieces(self, head, tail, index):
        nb = self.topo.nb
        specs = [pl.BlockSpec((head, None) + (1,) * nb + tail, lambda *g: index(g)[0] + (0,) * nb + index(g)[1])]
        for s in range(nb):
            at = (0,) * s + (1,) + (0,) * (nb - 1 - s)
            specs.append(pl.BlockSpec((head, None, None) + (2,) * s + (1,) * (nb - s) + tail,
                                      lambda *g, s=s, at=at: index(g)[0] + (s,) + at + index(g)[1]))
        return specs

    def tri_pieces(self):
        return self._pieces(self.topo.nq, (RB, self.kb), lambda g: ((0, 0), (g[0], g[1])))

    def side_pieces(self, side):
        return self._pieces(1, (self.rows, self.width), lambda g: ((g[0], side), (0, 0)))


def call(sh, name, body, grid, ins, in_specs, outs, out_specs, scratch, moving=None, cid=0, pace=None):
    topo = sh.topo
    steps = math.prod(grid)
    params = dict(vmem_limit_bytes=62 * 1024 * 1024)
    hbm = pl.BlockSpec(memory_space=pl.ANY)
    n_in, n_out = len(ins), len(outs)
    if moving is not None:
        ins, in_specs = list(ins) + [moving], list(in_specs) + [hbm]
        outs, out_specs = list(outs) + [sh.landing(moving)], list(out_specs) + [hbm]
        sems = pltpu.SemaphoreType.DMA((topo.nq, 2, topo.nb))
        scratch = list(scratch) + [sems, sems]
        params.update(collective_id=cid, has_side_effects=True)

    def kernel(*refs):
        topo.here()
        if moving is None:
            body(topo, *refs)
            return
        work = refs[:n_in] + refs[n_in + 1:n_in + 1 + n_out] + refs[n_in + n_out + 2:-2]
        ex = Exchange(topo, refs[n_in], refs[n_in + 1 + n_out], refs[-2], refs[-1])
        step = pl.program_id(0)
        for d, size in enumerate(grid[1:], 1):
            step = step * size + pl.program_id(d)

        @pl.when(step == 0)
        def _():
            ex.barrier()
            for sub in range(2):
                ex.start(sub, 0)
        moves = ex.moves()
        due = [max(1, int((i + 1) * pace)) if pace else steps for i in range(len(moves))]
        for g in range(1, steps):
            now = [m for m, d in zip(moves, due) if d == g]
            if now:
                pl.when(step == g)(lambda now=now: [m() for m in now] and None)
        body(topo, *work)

        @pl.when(step == steps - 1)
        def _():
            for m, d in zip(moves, due):
                if d >= steps:
                    m()
            ex.drain()

    return pl.pallas_call(kernel, grid=grid, out_shape=tuple(outs), in_specs=in_specs, out_specs=tuple(out_specs),
                          scratch_shapes=scratch, compiler_params=pltpu.CompilerParams(**params), name=name)(*ins)


def project(sh, z, m, norm, wp, **move):
    return call(sh, "project", _project_kernel, sh.grid, (z, m, norm, wp), [sh.z_spec, sh.m_spec, _whole(norm), _whole(wp)],
                [sh.sides], [sh.sides_spec], [sh.scr], **move)


def finish_project(sh, z, m, n0, mid, wg, wo, n1, wp, t, **move):
    flat = (n0, mid, wg, wo, n1, wp)
    return call(sh, "finish_project", _finish_project_kernel, sh.grid, (z, m) + flat + (t[0],) + (t[1],) * sh.topo.nb,
                [sh.z_spec, sh.m_spec] + [_whole(a) for a in flat] + sh.tri_pieces(),
                [sh.zt, sh.sides], [sh.zt_spec, sh.sides_spec], [sh.scr_y, sh.scr], **move)


def finish(sh, zt, n0, mid, wg, wo, t, **move):
    flat = (n0, mid, wg, wo)
    return call(sh, "finish", _finish_kernel, sh.grid, (zt,) + flat + (t[0],) + (t[1],) * sh.topo.nb,
                [sh.zt_spec] + [_whole(a) for a in flat] + sh.tri_pieces(),
                [jax.ShapeDtypeStruct((sh.rows, sh.width, sh.cz), BF16)], [sh.z_spec], [sh.scr_y], **move)


def triangle(sh, sides, contract, **move):
    nb = sh.topo.nb
    return call(sh, "triangle", lambda topo, *refs: _triangle_kernel(topo, contract, *refs), (sh.topo.nq,),
                ((sides[0],) + (sides[1],) * nb) * 2, sh.side_pieces(0) + sh.side_pieces(1),
                [sh.tri], [pl.BlockSpec((1, None) + sh.bits + (sh.rows, sh.width), lambda q: (q,) + (0,) * (nb + 3))],
                [sh.mat, sh.mat], **move)


def _lanes(norm):
    return jnp.broadcast_to(norm.astype(F32)[..., None], norm.shape + (LANES,))


def solution(mesh):
    n = mesh.shape["dap"]
    row_spec = P(("data", "dap"), None, None)
    mask_spec = P(("data", "dap"), None)
    rep = P()

    def per_device(z_one, mask_one, z_two, mask_two, norm_in, w_proj, w_gate, norm_mid, w_out):
        sh = Shapes(n, z_one, w_proj)
        nin, mid = _lanes(norm_in), _lanes(norm_mid)
        wp, wg, wo = (jnp.swapaxes(w, 1, 2) for w in (w_proj, w_gate, w_out))
        zs, ms = (z_one, z_two), (mask_one, mask_two)
        mask_a, mask_b = ms
        s1, = project(sh, zs[0], mask_a, nin[0], wp[0])
        s2, w1 = project(sh, zs[1], mask_b, nin[0], wp[0], moving=s1, cid=0)
        t1, w2 = triangle(sh, (s1, w1), 1, moving=s2, cid=1)
        t2, v1 = triangle(sh, (s2, w2), 1, moving=t1, cid=2)
        flat = (nin[0], mid[0], wg[0], wo[0], nin[1], wp[1])
        zt1, s1, v2 = finish_project(sh, zs[0], mask_a, *flat, (t1, v1), moving=t2, cid=3, pace=0.85)
        zt2, s2, w1 = finish_project(sh, zs[1], mask_b, *flat, (t2, v2), moving=s1, cid=4, pace=1.9)
        t1, w2 = triangle(sh, (s1, w1), 0, moving=s2, cid=5)
        t2, v1 = triangle(sh, (s2, w2), 0, moving=t1, cid=6)
        flat = (nin[1], mid[1], wg[1], wo[1])
        z1, v2 = finish(sh, zt1, *flat, (t1, v1), moving=t2, cid=7, pace=1.9)
        z2, = finish(sh, zt2, *flat, (t2, v2))
        return z1, z2

    return jax.shard_map(per_device, mesh=mesh,
                         in_specs=(row_spec, mask_spec, row_spec, mask_spec, rep, rep, rep, rep, rep),
                         out_specs=(row_spec, row_spec), check_vma=False)
```

```python
import functools
import math

import jax
import jax.numpy as jnp
from jax import lax
from jax.experimental import pallas as pl
from jax.experimental.pallas import tpu as pltpu
from jax.sharding import PartitionSpec as P

RB = 8
LANES = 128
UNROLL = 4
F32, BF16 = jnp.float32, jnp.bfloat16


def _norm_cols(v, gain, shift):
    mean = jnp.mean(v, axis=0, keepdims=True)
    cen = v - mean
    var = jnp.mean(cen * cen, axis=0, keepdims=True)
    return (cen * lax.rsqrt(var + 1e-5) * gain + shift).astype(BF16)


def _mm(a, b):
    return lax.dot_general(a, b, (((1,), (0,)), ((), ())), preferred_element_type=F32)


def _lane(kk):
    return slice(kk * LANES, (kk + 1) * LANES)


def _wide(v, width):
    return jnp.concatenate([v] * (width // LANES), axis=1)


def _project(z_t, norm_ref, wp_ref, scr, r):
    hid = wp_ref.shape[0] // 4
    width = z_t.shape[1]
    x_t = _norm_cols(z_t, _wide(norm_ref[0], width), _wide(norm_ref[1], width))
    q = _mm(wp_ref[...], x_t)
    for s in range(2):
        p, g = q[2 * s * hid:(2 * s + 1) * hid], q[(2 * s + 1) * hid:(2 * s + 2) * hid]
        v = jax.nn.sigmoid(g) * p
        for kk in range(width // LANES):
            scr[kk, pl.ds(s * hid * RB + r, hid, stride=RB), :] = v[:, _lane(kk)]


def _each_tile(width, f):
    def body(kk, c):
        f(kk, pl.ds(pl.multiple_of(kk * LANES, LANES), LANES))
        return c
    lax.fori_loop(0, width // LANES, body, 0)


def _emit_sides(scr, m_ref, out_ref, topo):
    half = scr.shape[1] // 2

    def tile(kk, lanes):
        keep = m_ref[:, lanes].astype(F32)
        for q in range(topo.nq):
            for s in range(2):
                for rho, owner in topo.blocks(topo.order(q, s)):
                    at = pl.multiple_of(s * half + (owner * topo.nq + q) * RB, RB)
                    out_ref[(q, s) + rho + (slice(None), lanes)] = (scr[kk, pl.ds(at, RB), :] * keep).astype(BF16)
    _each_tile(m_ref.shape[1], tile)


def _finish(z_t, r, scr_y, norm_ref, mid_ref, wg_ref, wo_ref):
    hid = wo_ref.shape[1]
    width = z_t.shape[1]
    x_t = _norm_cols(z_t, _wide(norm_ref[0], width), _wide(norm_ref[1], width))
    gate = jax.nn.sigmoid(_mm(wg_ref[...], x_t))
    y = [scr_y[kk, pl.ds(r, hid, stride=RB), :] for kk in range(width // LANES)]
    y = jnp.concatenate([(v * mid_ref[0] + mid_ref[1]).astype(BF16) for v in y], axis=1)
    return (z_t + gate * _mm(wo_ref[...], y)).astype(BF16)


def _norm_mid(t_refs, scr_y, topo):
    tiles = [(q,) + rest for q in range(topo.nq) for rest in topo.landed(topo.order(q, 0))]
    inv_n = 1.0 / len(tiles)

    def tile(kk, lanes):
        def load(t):
            return t_refs[t[1]][(t[0],) + t[2] + (slice(None), lanes)].astype(F32)

        def total(f):
            part = [f(load(t)) for t in tiles[:4]]
            for i, t in enumerate(tiles[4:]):
                part[i % 4] = part[i % 4] + f(load(t))
            return (part[0] + part[1]) + (part[2] + part[3])
        mean = total(lambda v: v) * inv_n
        inv = lax.rsqrt(total(lambda v: (v - mean) * (v - mean)) * inv_n + 1e-5)
        for t in tiles:
            at = pl.multiple_of((t[3] * topo.nq + t[0]) * RB, RB)
            scr_y[kk, pl.ds(at, RB), :] = (load(t) - mean) * inv
    _each_tile(scr_y.shape[0] * LANES, tile)


def _row_loop(f):
    def body(i, c):
        for u in range(UNROLL):
            f(i * UNROLL + u)
        return c
    lax.fori_loop(0, RB // UNROLL, body, 0)


class Topo:
    def __init__(self, n):
        self.side = math.isqrt(n // 2)
        ring = self.side.bit_length() - 1
        self.nq = 2 * ring
        self.nb = self.nq + 1
        self.links = [(axis, bit) for bit in range(ring) for axis in ("x", "y")]
        self.weight = {("core", 0): 1}
        self.weight.update({("x", b): 2 << b for b in range(ring)})
        self.weight.update({("y", b): (2 << ring) << b for b in range(ring)})

    def order(self, q, core_first):
        links = [self.links[(q + i) % self.nq] for i in range(self.nq)]
        return [("core", 0)] + links if core_first else links + [("core", 0)]

    def here(self):
        me = lax.axis_index("dap")
        self.pos = {"core": lax.rem(me, 2), "x": lax.rem(me // 2, self.side), "y": me // (2 * self.side)}
        self.bit = {}
        for axis, b in self.weight:
            v = self.pos[axis]
            self.bit[axis, b] = lax.rem(v // (1 << b) + v // (2 << b), 2) if axis != "core" else v
        return self

    def neighbour(self, link):
        axis, b = link
        pos = dict(self.pos)
        v, span = pos[axis], 2 << b
        pos[axis] = v - lax.rem(v, span) + (span - 1) - lax.rem(v, span)
        return (pos["y"] * self.side + pos["x"]) * 2 + pos["core"]

    def partner(self, q, core_first, s):
        at = s - 1 if core_first else s
        if at < 0 or at >= self.nq:
            return self.neighbour(("core", 0))
        i = lax.rem(q + at, self.nq)
        hit = [jnp.where(i == k, self.neighbour(link), 0) for k, link in enumerate(self.links)]
        return functools.reduce(lambda u, v: u + v, hit)

    def blocks(self, order):
        out = [((), 0)]
        for link in order:
            w, own = self.weight[link], self.bit[link]
            out = [(r + (f,), o + w * (1 - own if f else own)) for r, o in out for f in (0, 1)]
        return out

    def landed(self, order):
        out = []
        for rho, owner in self.blocks(order):
            last = max([i for i, f in enumerate(rho) if f], default=-1)
            idx = (0,) * self.nb if last < 0 else rho[:last] + (0,) * (self.nb - last)
            out.append((last + 1, idx, owner))
        return out

    def natural(self, owner):
        side, core, rest = self.side, lax.rem(owner, 2), owner // 2
        gx, gy = lax.rem(rest, side), rest // side

        def binary(g):
            v, b = 0, 0
            k = side.bit_length() - 2
            for i in range(k, -1, -1):
                b = lax.rem(b + lax.rem(g // (1 << i), 2), 2)
                v = v + b * (1 << i)
            return v
        return (binary(gy) * side + binary(gx)) * 2 + core

    def gray_bits(self, p):
        pos = {"core": p % 2, "x": p // 2 % self.side, "y": p // 2 // self.side}
        return {k: (pos[k[0]] if k[0] == "core" else (pos[k[0]] >> k[1] ^ pos[k[0]] >> (k[1] + 1)) & 1) for k in self.weight}

    def relative(self, order, p):
        bits = self.gray_bits(p)
        return tuple((1 - self.bit[k]) if bits[k] else self.bit[k] for k in order)


class Exchange:
    def __init__(self, topo, src, dst, ssem, rsem):
        self.topo, self.src, self.dst, self.ssem, self.rsem = topo, src, dst, ssem, rsem
        self.cut = src.shape[1] == 1

    def _tail(self, sub):
        if not self.cut:
            return sub, ()
        w = self.src.shape[-1] // 2
        return 0, (slice(None), pl.ds(sub * w, w))

    def _first(self, sub):
        return sub == 1 and not self.cut

    def _copy(self, q, sub, s, a, b):
        return pltpu.make_async_remote_copy(
            src_ref=a, dst_ref=b, send_sem=self.ssem.at[q, sub, s], recv_sem=self.rsem.at[q, sub, s],
            device_id={"dap": self.topo.partner(q, self._first(sub), s)}, device_id_type=pl.DeviceIdType.MESH)

    def _streams(self, f):
        def body(q, c):
            f(q)
            return c
        lax.fori_loop(0, self.topo.nq, body, 0)

    def start(self, sub, s):
        nb, free = self.topo.nb, (slice(None),)
        k, tail = self._tail(sub)

        def stream(q):
            for t in range(-1, s):
                if t < 0:
                    idx = (0,) * s + (1,) + free * (nb - 1 - s) + tail
                    a = self.src.at[(q, k) + idx]
                else:
                    idx = free * t + (1,) + (0,) * (s - 1 - t) + (1,) + free * (nb - 1 - s) + tail
                    a = self.dst.at[(q, k, t) + idx]
                self._copy(q, sub, s, a, self.dst.at[(q, k, s) + idx]).start()
        self._streams(stream)

    def _whole(self, q, sub, s):
        k, tail = self._tail(sub)
        ref = self.dst.at[(q, k, s) + (slice(None),) * s + (1,) + (slice(None),) * (self.topo.nb - 1 - s) + tail]
        return self._copy(q, sub, s, ref, ref)

    def arrive(self, sub, s):
        self._streams(lambda q: self._whole(q, sub, s).wait_recv())

    def drain(self):
        for sub in range(2):
            for s in range(self.topo.nb):
                self._streams(lambda q, sub=sub, s=s: self._whole(q, sub, s).wait_send())

    def barrier(self):
        bar = pltpu.get_barrier_semaphore()
        for link in self.topo.weight:
            pl.semaphore_signal(bar, inc=1, device_id={"dap": self.topo.neighbour(link)}, device_id_type=pl.DeviceIdType.MESH)
        pl.semaphore_wait(bar, len(self.topo.weight))

    def moves(self):
        out = []
        for s in range(self.topo.nb):
            for sub in (range(2) if self.cut else (1, 0)):
                def move(s=s, sub=sub):
                    self.arrive(sub, s)
                    if s + 1 < self.topo.nb:
                        self.start(sub, s + 1)
                out.append((2 * s + (sub + 1 if self.cut else 0.4 if sub and s == 0 else 1 - sub), move))
        return out


def _project_kernel(topo, z_ref, m_ref, norm_ref, wp_ref, out_ref, scr):
    _row_loop(lambda r: _project(z_ref[r].astype(F32).T, norm_ref, wp_ref, scr, r))
    _emit_sides(scr, m_ref, out_ref, topo)


def _finish_project_kernel(topo, z_ref, m_ref, n0_ref, mid_ref, wg_ref, wo_ref, n1_ref, wp_ref, *refs):
    t_refs, (zt_ref, out_ref, scr_y, scr) = refs[:-4], refs[-4:]
    _norm_mid(t_refs, scr_y, topo)

    def row(r):
        z_new = _finish(z_ref[r].astype(F32).T, r, scr_y, n0_ref, mid_ref, wg_ref, wo_ref)
        zt_ref[r] = z_new
        _project(z_new.astype(F32), n1_ref, wp_ref, scr, r)
    _row_loop(row)
    _emit_sides(scr, m_ref, out_ref, topo)


def _finish_kernel(topo, zt_ref, n0_ref, mid_ref, wg_ref, wo_ref, *refs):
    t_refs, (z_ref, scr_y) = refs[:-2], refs[-2:]
    _norm_mid(t_refs, scr_y, topo)

    def row(r):
        z_new = _finish(zt_ref[r].astype(F32), r, scr_y, n0_ref, mid_ref, wg_ref, wo_ref)
        z_ref[r] = z_new.astype(F32).T.astype(BF16)
    _row_loop(row)


def _triangle_kernel(topo, contract, *refs):
    half = (len(refs) - 3) // 2
    a_refs, b_refs, (out_ref, a_scr, b_scr) = refs[:half], refs[half:2 * half], refs[-3:]
    n, rows, width = a_scr.shape
    step = pl.program_id(0)

    def gather(q):
        a_order, b_order = topo.order(q, 0), topo.order(q, 1)
        rhos = [dict(zip(a_order, rho)) for rho, _ in topo.blocks(a_order)]
        for i, (piece, idx, _) in enumerate(topo.landed(a_order)):
            a_scr[i] = a_refs[piece][(0,) + idx]
        for (rho, owner), (piece, idx, _) in zip(topo.blocks(b_order), topo.landed(b_order)):
            at = topo.natural(owner) if contract else rhos.index(dict(zip(b_order, rho)))
            b_scr[at] = b_refs[piece][(0,) + idx]

    def scatter(q):
        for p in range(n):
            out_ref[(0,) + topo.relative(topo.order(q, 0), p)] = a_scr[p]
    for q in range(topo.nq):
        pl.when(step == q)(functools.partial(gather, q))
    a, b = a_scr[...].reshape(n * rows, width), b_scr[...].reshape(n * rows, width)
    t = lax.dot_general(a, b, (((contract,), (contract,)), ((), ())), preferred_element_type=F32)
    t = t.astype(BF16).reshape(n, rows, width)
    if contract:
        out_ref[...] = t.reshape(out_ref.shape)
    else:
        a_scr[...] = t
        for q in range(topo.nq):
            pl.when(step == q)(functools.partial(scatter, q))


def _whole(a):
    return pl.BlockSpec(a.shape, lambda *_: (0,) * a.ndim)


class Shapes:
    def __init__(self, n, z, w_proj):
        self.topo = topo = Topo(n)
        self.n, (self.rows, self.width, self.cz) = n, z.shape
        self.hid = w_proj.shape[-1] // 4
        assert self.hid == n * topo.nq
        self.kb = 2 * LANES if self.width % (2 * LANES) == 0 else LANES
        self.grid = (self.rows // RB, self.width // self.kb)
        self.bits = (2,) * topo.nb
        zero = (0,) * topo.nb
        self.z_spec = pl.BlockSpec((RB, self.kb, self.cz), lambda i, j: (i, j, 0))
        self.zt_spec = pl.BlockSpec((RB, self.cz, self.kb), lambda i, j: (i, 0, j))
        self.m_spec = pl.BlockSpec((RB, self.kb), lambda i, j: (i, j))
        self.sides_spec = pl.BlockSpec((topo.nq, 2) + self.bits + (RB, self.kb), lambda i, j: (0, 0) + zero + (i, j))
        self.sides = jax.ShapeDtypeStruct((topo.nq, 2) + self.bits + (self.rows, self.width), BF16)
        self.tri = jax.ShapeDtypeStruct((topo.nq, 1) + self.bits + (self.rows, self.width), BF16)
        self.zt = jax.ShapeDtypeStruct((self.rows, self.cz, self.width), BF16)
        self.scr = pltpu.VMEM((self.kb // LANES, 2 * self.hid * RB, LANES), F32)
        self.scr_y = pltpu.VMEM((self.kb // LANES, self.hid * RB, LANES), F32)
        self.mat = pltpu.VMEM((n, self.rows, self.width), BF16)

    def landing(self, src):
        return jax.ShapeDtypeStruct(src.shape[:2] + (self.topo.nb,) + src.shape[2:], BF16)

    def _pieces(self, head, tail, index):
        nb = self.topo.nb
        specs = [pl.BlockSpec((head, None) + (1,) * nb + tail, lambda *g: index(g)[0] + (0,) * nb + index(g)[1])]
        for s in range(nb):
            at = (0,) * s + (1,) + (0,) * (nb - 1 - s)
            specs.append(pl.BlockSpec((head, None, None) + (2,) * s + (1,) * (nb - s) + tail,
                                      lambda *g, s=s, at=at: index(g)[0] + (s,) + at + index(g)[1]))
        return specs

    def tri_pieces(self):
        return self._pieces(self.topo.nq, (RB, self.kb), lambda g: ((0, 0), (g[0], g[1])))

    def side_pieces(self, side):
        return self._pieces(1, (self.rows, self.width), lambda g: ((g[0], side), (0, 0)))


def call(sh, name, body, grid, ins, in_specs, outs, out_specs, scratch, moving=None, cid=0, pace=None):
    topo = sh.topo
    steps = math.prod(grid)
    params = dict(vmem_limit_bytes=62 * 1024 * 1024)
    hbm = pl.BlockSpec(memory_space=pl.ANY)
    n_in, n_out = len(ins), len(outs)
    if moving is not None:
        ins, in_specs = list(ins) + [moving], list(in_specs) + [hbm]
        outs, out_specs = list(outs) + [sh.landing(moving)], list(out_specs) + [hbm]
        sems = pltpu.SemaphoreType.DMA((topo.nq, 2, topo.nb))
        scratch = list(scratch) + [sems, sems]
        params.update(collective_id=cid, has_side_effects=True)

    def kernel(*refs):
        topo.here()
        if moving is None:
            body(topo, *refs)
            return
        work = refs[:n_in] + refs[n_in + 1:n_in + 1 + n_out] + refs[n_in + n_out + 2:-2]
        ex = Exchange(topo, refs[n_in], refs[n_in + 1 + n_out], refs[-2], refs[-1])
        step = pl.program_id(0)
        for d, size in enumerate(grid[1:], 1):
            step = step * size + pl.program_id(d)

        @pl.when(step == 0)
        def _():
            ex.barrier()
            for sub in range(2):
                ex.start(sub, 0)
        moves = ex.moves()
        due = [(max(1, round(t * pace)) if pace else steps, m) for t, m in moves]
        for g in range(1, steps):
            now = [m for d, m in due if d == g]
            if now:
                pl.when(step == g)(lambda now=now: [m() for m in now] and None)
        body(topo, *work)

        @pl.when(step == steps - 1)
        def _():
            for d, m in due:
                if d >= steps:
                    m()
            ex.drain()

    return pl.pallas_call(kernel, grid=grid, out_shape=tuple(outs), in_specs=in_specs, out_specs=tuple(out_specs),
                          scratch_shapes=scratch, compiler_params=pltpu.CompilerParams(**params), name=name)(*ins)


def project(sh, z, m, norm, wp, **move):
    return call(sh, "project", _project_kernel, sh.grid, (z, m, norm, wp), [sh.z_spec, sh.m_spec, _whole(norm), _whole(wp)],
                [sh.sides], [sh.sides_spec], [sh.scr], **move)


def finish_project(sh, z, m, n0, mid, wg, wo, n1, wp, t, **move):
    flat = (n0, mid, wg, wo, n1, wp)
    return call(sh, "finish_project", _finish_project_kernel, sh.grid, (z, m) + flat + (t[0],) + (t[1],) * sh.topo.nb,
                [sh.z_spec, sh.m_spec] + [_whole(a) for a in flat] + sh.tri_pieces(),
                [sh.zt, sh.sides], [sh.zt_spec, sh.sides_spec], [sh.scr_y, sh.scr], **move)


def finish(sh, zt, n0, mid, wg, wo, t, **move):
    flat = (n0, mid, wg, wo)
    return call(sh, "finish", _finish_kernel, sh.grid, (zt,) + flat + (t[0],) + (t[1],) * sh.topo.nb,
                [sh.zt_spec] + [_whole(a) for a in flat] + sh.tri_pieces(),
                [jax.ShapeDtypeStruct((sh.rows, sh.width, sh.cz), BF16)], [sh.z_spec], [sh.scr_y], **move)


def triangle(sh, sides, contract, **move):
    nb = sh.topo.nb
    return call(sh, "triangle", lambda topo, *refs: _triangle_kernel(topo, contract, *refs), (sh.topo.nq,),
                ((sides[0],) + (sides[1],) * nb) * 2, sh.side_pieces(0) + sh.side_pieces(1),
                [sh.tri], [pl.BlockSpec((1, None) + sh.bits + (sh.rows, sh.width), lambda q: (q,) + (0,) * (nb + 3))],
                [sh.mat, sh.mat], **move)


def _lanes(norm):
    return jnp.broadcast_to(norm.astype(F32)[..., None], norm.shape + (LANES,))


def solution(mesh):
    n = mesh.shape["dap"]
    row_spec = P(("data", "dap"), None, None)
    mask_spec = P(("data", "dap"), None)
    rep = P()

    def per_device(z_one, mask_one, z_two, mask_two, norm_in, w_proj, w_gate, norm_mid, w_out):
        sh = Shapes(n, z_one, w_proj)
        nin, mid = _lanes(norm_in), _lanes(norm_mid)
        wp, wg, wo = (jnp.swapaxes(w, 1, 2) for w in (w_proj, w_gate, w_out))
        zs, ms = (z_one, z_two), (mask_one, mask_two)
        mask_a, mask_b = ms
        s1, = project(sh, zs[0], mask_a, nin[0], wp[0])
        s2, w1 = project(sh, zs[1], mask_b, nin[0], wp[0], moving=s1, cid=0, pace=5.5)
        t1, w2 = triangle(sh, (s1, w1), 1, moving=s2, cid=1)
        t2, v1 = triangle(sh, (s2, w2), 1, moving=t1, cid=2)
        flat = (nin[0], mid[0], wg[0], wo[0], nin[1], wp[1])
        zt1, s1, v2 = finish_project(sh, zs[0], mask_a, *flat, (t1, v1), moving=t2, cid=3, pace=1.6)
        zt2, s2, w1 = finish_project(sh, zs[1], mask_b, *flat, (t2, v2), moving=s1, cid=4, pace=3.2)
        t1, w2 = triangle(sh, (s1, w1), 0, moving=s2, cid=5)
        t2, v1 = triangle(sh, (s2, w2), 0, moving=t1, cid=6)
        flat = (nin[1], mid[1], wg[1], wo[1])
        z1, v2 = finish(sh, zt1, *flat, (t1, v1), moving=t2, cid=7, pace=3.4)
        z2, = finish(sh, zt2, *flat, (t2, v2))
        return z1, z2

    return jax.shard_map(per_device, mesh=mesh,
                         in_specs=(row_spec, mask_spec, row_spec, mask_spec, rep, rep, rep, rep, rep),
                         out_specs=(row_spec, row_spec), check_vma=False)
```

```python
import functools
import math

import jax
import jax.numpy as jnp
from jax import lax
from jax.experimental import pallas as pl
from jax.experimental.pallas import tpu as pltpu
from jax.sharding import PartitionSpec as P

RB = 8
LANES = 128
UNROLL = 4
F32, BF16 = jnp.float32, jnp.bfloat16


def _norm_cols(v, gain, shift):
    mean = jnp.mean(v, axis=0, keepdims=True)
    cen = v - mean
    var = jnp.mean(cen * cen, axis=0, keepdims=True)
    return (cen * lax.rsqrt(var + 1e-5) * gain + shift).astype(BF16)


def _mm(a, b):
    return lax.dot_general(a, b, (((1,), (0,)), ((), ())), preferred_element_type=F32)


def _project(z_t, norm_ref, wp_ref, scr, r, kk):
    hid = wp_ref.shape[0] // 4
    q = _mm(wp_ref[...], _norm_cols(z_t, norm_ref[0], norm_ref[1]))
    for s in range(2):
        p, g = q[2 * s * hid:(2 * s + 1) * hid], q[(2 * s + 1) * hid:(2 * s + 2) * hid]
        scr[kk, pl.ds(s * hid * RB + r, hid, stride=RB), :] = jax.nn.sigmoid(g) * p


def _each_tile(width, f):
    def body(kk, c):
        f(kk, pl.ds(pl.multiple_of(kk * LANES, LANES), LANES))
        return c
    lax.fori_loop(0, width // LANES, body, 0)


def _emit_sides(scr, m_ref, out_ref, topo):
    half = scr.shape[1] // 2

    def tile(kk, lanes):
        keep = m_ref[:, lanes].astype(F32)
        for q in range(topo.nq):
            for s in range(2):
                for rho, owner in topo.blocks(topo.order(q)):
                    at = pl.multiple_of(s * half + (owner * topo.nq + q) * RB, RB)
                    out_ref[(q, s) + rho + (slice(None), lanes)] = (scr[kk, pl.ds(at, RB), :] * keep).astype(BF16)
    _each_tile(m_ref.shape[1], tile)


def _finish(z_t, r, kk, scr_y, norm_ref, mid_ref, wg_ref, wo_ref):
    hid = wo_ref.shape[1]
    gate = jax.nn.sigmoid(_mm(wg_ref[...], _norm_cols(z_t, norm_ref[0], norm_ref[1])))
    y = scr_y[kk, pl.ds(r, hid, stride=RB), :]
    y = (y * mid_ref[0] + mid_ref[1]).astype(BF16)
    return (z_t + gate * _mm(wo_ref[...], y)).astype(BF16)


def _norm_mid(t_refs, scr_y, topo):
    tiles = [(q,) + rest for q in range(topo.nq) for rest in topo.landed(topo.order(q))]
    inv_n = 1.0 / len(tiles)

    def tile(kk, lanes):
        def load(t):
            return t_refs[t[1]][(t[0],) + t[2] + (slice(None), lanes)].astype(F32)

        def total(f):
            part = [f(load(t)) for t in tiles[:4]]
            for i, t in enumerate(tiles[4:]):
                part[i % 4] = part[i % 4] + f(load(t))
            return (part[0] + part[1]) + (part[2] + part[3])
        mean = total(lambda v: v) * inv_n
        inv = lax.rsqrt(total(lambda v: (v - mean) * (v - mean)) * inv_n + 1e-5)
        for t in tiles:
            at = pl.multiple_of((t[3] * topo.nq + t[0]) * RB, RB)
            scr_y[kk, pl.ds(at, RB), :] = (load(t) - mean) * inv
    _each_tile(scr_y.shape[0] * LANES, tile)


def _row_loop(width, f):
    def body(i, c):
        for u in range(UNROLL):
            for kk in range(width // LANES):
                f(i * UNROLL + u, kk, slice(kk * LANES, (kk + 1) * LANES))
        return c
    lax.fori_loop(0, RB // UNROLL, body, 0)


class Topo:
    def __init__(self, n):
        self.side = math.isqrt(n // 2)
        ring = self.side.bit_length() - 1
        self.nq = 2 * ring
        self.nb = self.nq + 1
        self.links = [(axis, bit) for bit in range(ring) for axis in ("x", "y")]
        self.weight = {("core", 0): 1}
        self.weight.update({("x", b): 2 << b for b in range(ring)})
        self.weight.update({("y", b): (2 << ring) << b for b in range(ring)})

    def order(self, q):
        links = [self.links[(q + i) % self.nq] for i in range(self.nq)]
        return links[:self.nq // 2] + [("core", 0)] + links[self.nq // 2:]

    def here(self):
        me = lax.axis_index("dap")
        self.pos = {"core": lax.rem(me, 2), "x": lax.rem(me // 2, self.side), "y": me // (2 * self.side)}
        self.bit = {}
        for axis, b in self.weight:
            v = self.pos[axis]
            self.bit[axis, b] = lax.rem(v // (1 << b) + v // (2 << b), 2) if axis != "core" else v
        return self

    def neighbour(self, link):
        axis, b = link
        pos = dict(self.pos)
        v, span = pos[axis], 2 << b
        pos[axis] = v - lax.rem(v, span) + (span - 1) - lax.rem(v, span)
        return (pos["y"] * self.side + pos["x"]) * 2 + pos["core"]

    def partner(self, q, s):
        if s == self.nq // 2:
            return self.neighbour(("core", 0))
        at = s if s < self.nq // 2 else s - 1
        i = lax.rem(q + at, self.nq)
        hit = [jnp.where(i == k, self.neighbour(link), 0) for k, link in enumerate(self.links)]
        return functools.reduce(lambda u, v: u + v, hit)

    def blocks(self, order):
        out = [((), 0)]
        for link in order:
            w, own = self.weight[link], self.bit[link]
            out = [(r + (f,), o + w * (1 - own if f else own)) for r, o in out for f in (0, 1)]
        return out

    def landed(self, order):
        out = []
        for rho, owner in self.blocks(order):
            last = max([i for i, f in enumerate(rho) if f], default=-1)
            idx = (0,) * self.nb if last < 0 else rho[:last] + (0,) * (self.nb - last)
            out.append((last + 1, idx, owner))
        return out

    def natural(self, owner):
        side, core, rest = self.side, lax.rem(owner, 2), owner // 2
        gx, gy = lax.rem(rest, side), rest // side

        def binary(g):
            v, b = 0, 0
            k = side.bit_length() - 2
            for i in range(k, -1, -1):
                b = lax.rem(b + lax.rem(g // (1 << i), 2), 2)
                v = v + b * (1 << i)
            return v
        return (binary(gy) * side + binary(gx)) * 2 + core

    def gray_bits(self, p):
        pos = {"core": p % 2, "x": p // 2 % self.side, "y": p // 2 // self.side}
        return {k: (pos[k[0]] if k[0] == "core" else (pos[k[0]] >> k[1] ^ pos[k[0]] >> (k[1] + 1)) & 1) for k in self.weight}

    def relative(self, order, p):
        bits = self.gray_bits(p)
        return tuple((1 - self.bit[k]) if bits[k] else self.bit[k] for k in order)


class Exchange:
    def __init__(self, topo, src, dst, ssem, rsem):
        self.topo, self.src, self.dst, self.ssem, self.rsem = topo, src, dst, ssem, rsem
        self.cut = src.shape[1] == 1

    def _tail(self, sub):
        if not self.cut:
            return sub, ()
        w = self.src.shape[-1] // 2
        return 0, (slice(None), pl.ds(sub * w, w))

    def _copy(self, q, sub, s, a, b):
        return pltpu.make_async_remote_copy(
            src_ref=a, dst_ref=b, send_sem=self.ssem.at[q, sub, s], recv_sem=self.rsem.at[q, sub, s],
            device_id={"dap": self.topo.partner(q, s)}, device_id_type=pl.DeviceIdType.MESH)

    def _streams(self, f):
        def body(q, c):
            f(q)
            return c
        lax.fori_loop(0, self.topo.nq, body, 0)

    def start(self, sub, s):
        nb, free = self.topo.nb, (slice(None),)
        k, tail = self._tail(sub)

        def stream(q):
            for t in range(-1, s):
                if t < 0:
                    idx = (0,) * s + (1,) + free * (nb - 1 - s) + tail
                    a = self.src.at[(q, k) + idx]
                else:
                    idx = free * t + (1,) + (0,) * (s - 1 - t) + (1,) + free * (nb - 1 - s) + tail
                    a = self.dst.at[(q, k, t) + idx]
                self._copy(q, sub, s, a, self.dst.at[(q, k, s) + idx]).start()
        self._streams(stream)

    def _whole(self, q, sub, s):
        k, tail = self._tail(sub)
        ref = self.dst.at[(q, k, s) + (slice(None),) * s + (1,) + (slice(None),) * (self.topo.nb - 1 - s) + tail]
        return self._copy(q, sub, s, ref, ref)

    def arrive(self, sub, s):
        self._streams(lambda q: self._whole(q, sub, s).wait_recv())

    def drain(self):
        for sub in range(2):
            for s in range(self.topo.nb):
                self._streams(lambda q, sub=sub, s=s: self._whole(q, sub, s).wait_send())

    def barrier(self):
        bar = pltpu.get_barrier_semaphore()
        for link in self.topo.weight:
            pl.semaphore_signal(bar, inc=1, device_id={"dap": self.topo.neighbour(link)}, device_id_type=pl.DeviceIdType.MESH)
        pl.semaphore_wait(bar, len(self.topo.weight))

    def moves(self):
        mid, out = self.topo.nq // 2, []
        for s in range(self.topo.nb):
            for sub in range(2):
                def move(s=s, sub=sub):
                    self.arrive(sub, s)
                    if s + 1 < self.topo.nb:
                        self.start(sub, s + 1)
                out.append((2 * s + sub + 1 if s < mid else 2 * s + sub - 0.5 if s == mid else 2 * s + sub - 1, move))
        return sorted(out, key=lambda m: m[0])


def _project_kernel(topo, norm, wp, z_ref, m_ref, out_ref, scr):
    def row(r, kk, lanes):
        _project(z_ref[r, lanes, :].astype(F32).T, norm, wp, scr, r, kk)
    _row_loop(z_ref.shape[1], row)
    _emit_sides(scr, m_ref, out_ref, topo)


def _finish_project_kernel(topo, n0, mid, wg, wo, n1, wp, z_ref, m_ref, *refs):
    t_refs, (zt_ref, out_ref, scr_y, scr) = refs[:-4], refs[-4:]
    _norm_mid(t_refs, scr_y, topo)

    def row(r, kk, lanes):
        z_new = _finish(z_ref[r, lanes, :].astype(F32).T, r, kk, scr_y, n0, mid, wg, wo)
        zt_ref[r, :, lanes] = z_new
        _project(z_new.astype(F32), n1, wp, scr, r, kk)
    _row_loop(z_ref.shape[1], row)
    _emit_sides(scr, m_ref, out_ref, topo)


def _finish_kernel(topo, n0, mid, wg, wo, zt_ref, *refs):
    t_refs, (z_ref, scr_y) = refs[:-2], refs[-2:]
    _norm_mid(t_refs, scr_y, topo)

    def row(r, kk, lanes):
        z_new = _finish(zt_ref[r, :, lanes].astype(F32), r, kk, scr_y, n0, mid, wg, wo)
        z_ref[r, lanes, :] = z_new.astype(F32).T.astype(BF16)
    _row_loop(z_ref.shape[1], row)


def _finish_last_kernel(topo, n0, mid, wg, wo, zt_ref, other_ref, *refs):
    t_refs, (z_ref, other_out, scr_y) = refs[:-3], refs[-3:]
    other_out[...] = other_ref[...]
    _finish_kernel(topo, n0, mid, wg, wo, zt_ref, *t_refs, z_ref, scr_y)


def _triangle_kernel(topo, contract, *refs):
    half = (len(refs) - 3) // 2
    a_refs, b_refs, (out_ref, a_scr, b_scr) = refs[:half], refs[half:2 * half], refs[-3:]
    n, rows, width = a_scr.shape
    step = pl.program_id(0)

    def gather(q):
        for i, (piece, idx, owner) in enumerate(topo.landed(topo.order(q))):
            a_scr[i] = a_refs[piece][(0,) + idx]
            b_scr[topo.natural(owner) if contract else i] = b_refs[piece][(0,) + idx]

    def scatter(q):
        for p in range(n):
            out_ref[(0,) + topo.relative(topo.order(q), p)] = a_scr[p]
    for q in range(topo.nq):
        pl.when(step == q)(functools.partial(gather, q))
    a, b = a_scr[...].reshape(n * rows, width), b_scr[...].reshape(n * rows, width)
    t = lax.dot_general(a, b, (((contract,), (contract,)), ((), ())), preferred_element_type=F32)
    t = t.astype(BF16).reshape(n, rows, width)
    if contract:
        out_ref[...] = t.reshape(out_ref.shape)
    else:
        a_scr[...] = t
        for q in range(topo.nq):
            pl.when(step == q)(functools.partial(scatter, q))


def _whole(a):
    return pl.BlockSpec(a.shape, lambda *_: (0,) * a.ndim)


class Shapes:
    def __init__(self, n, z, w_proj):
        self.topo = topo = Topo(n)
        self.n, (self.rows, self.width, self.cz) = n, z.shape
        self.hid = w_proj.shape[-1] // 4
        assert self.hid == n * topo.nq
        self.kb = 2 * LANES if self.width % (2 * LANES) == 0 else LANES
        self.grid = (self.rows // RB, self.width // self.kb)
        self.bits = (2,) * topo.nb
        zero = (0,) * topo.nb
        self.z_spec = pl.BlockSpec((RB, self.kb, self.cz), lambda i, j: (i, j, 0))
        self.zt_spec = pl.BlockSpec((RB, self.cz, self.kb), lambda i, j: (i, 0, j))
        self.m_spec = pl.BlockSpec((RB, self.kb), lambda i, j: (i, j))
        self.sides_spec = pl.BlockSpec((topo.nq, 2) + self.bits + (RB, self.kb), lambda i, j: (0, 0) + zero + (i, j))
        self.sides = jax.ShapeDtypeStruct((topo.nq, 2) + self.bits + (self.rows, self.width), BF16)
        self.tri = jax.ShapeDtypeStruct((topo.nq, 1) + self.bits + (self.rows, self.width), BF16)
        self.z_out = jax.ShapeDtypeStruct(z.shape, BF16)
        self.zt = jax.ShapeDtypeStruct((self.rows, self.cz, self.width), BF16)
        self.scr = pltpu.VMEM((self.kb // LANES, 2 * self.hid * RB, LANES), F32)
        self.scr_y = pltpu.VMEM((self.kb // LANES, self.hid * RB, LANES), F32)
        self.mat = pltpu.VMEM((n, self.rows, self.width), BF16)

    def landing(self, src):
        return jax.ShapeDtypeStruct(src.shape[:2] + (self.topo.nb,) + src.shape[2:], BF16)

    def _pieces(self, head, tail, index):
        nb = self.topo.nb
        specs = [pl.BlockSpec((head, None) + (1,) * nb + tail, lambda *g: index(g)[0] + (0,) * nb + index(g)[1])]
        for s in range(nb):
            at = (0,) * s + (1,) + (0,) * (nb - 1 - s)
            specs.append(pl.BlockSpec((head, None, None) + (2,) * s + (1,) * (nb - s) + tail,
                                      lambda *g, s=s, at=at: index(g)[0] + (s,) + at + index(g)[1]))
        return specs

    def tri_pieces(self):
        return self._pieces(self.topo.nq, (RB, self.kb), lambda g: ((0, 0), (g[0], g[1])))

    def side_pieces(self, side):
        return self._pieces(1, (self.rows, self.width), lambda g: ((g[0], side), (0, 0)))


def _prepare(raw, ready, update):
    if len(ready.shape) == 3:
        for i in range(2):
            row = raw[update, i:i + 1, :].astype(F32)
            ready[i] = jnp.broadcast_to(row, (LANES, row.shape[1])).T
    else:
        ready[...] = raw[update].astype(F32).T.astype(BF16)


def call(sh, name, body, grid, params, ins, in_specs, outs, out_specs, scratch, moving=None, cid=0, pace=None):
    topo = sh.topo
    steps = math.prod(grid)
    compiler = dict(vmem_limit_bytes=62 * 1024 * 1024)
    hbm = pl.BlockSpec(memory_space=pl.ANY)
    n_par, n_in, n_out = len(params), len(ins), len(outs)
    ready = [pltpu.VMEM((2, p.shape[-1], LANES), F32) if p.shape[1] == 2 else pltpu.VMEM(p.shape[:0:-1], BF16) for p, _ in params]
    ins, in_specs = [p for p, _ in params] + list(ins), [_whole(p) for p, _ in params] + list(in_specs)
    scratch, sems = ready + list(scratch), []
    if moving is not None:
        ins, in_specs = ins + [moving], in_specs + [hbm]
        outs, out_specs = list(outs) + [sh.landing(moving)], list(out_specs) + [hbm]
        sems = [pltpu.SemaphoreType.DMA((topo.nq, 2, topo.nb))] * 2
        compiler.update(collective_id=cid, has_side_effects=True)
    n_move = len(sems) // 2

    def kernel(*refs):
        topo.here()
        raw, refs = refs[:n_par], refs[n_par:]
        work_in, refs = refs[:n_in], refs[n_in:]
        src, refs = refs[:n_move], refs[n_move:]
        work_out, refs = refs[:n_out], refs[n_out:]
        dst, refs = refs[:n_move], refs[n_move:]
        done, work_scr, sem_refs = refs[:n_par], refs[n_par:len(refs) - 2 * n_move], refs[len(refs) - 2 * n_move:]
        step = pl.program_id(0)
        for d, size in enumerate(grid[1:], 1):
            step = step * size + pl.program_id(d)
        due = []
        if n_move:
            ex = Exchange(topo, src[0], dst[0], *sem_refs)
            due = [(max(1, round(t * pace)) if pace else steps, m) for t, m in ex.moves()]

        @pl.when(step == 0)
        def _():
            if n_move:
                ex.barrier()
                for sub in range(2):
                    ex.start(sub, 0)
            for a, b, (_, update) in zip(raw, done, params):
                _prepare(a, b, update)
        for g in range(1, steps):
            now = [m for d, m in due if d == g]
            if now:
                pl.when(step == g)(lambda now=now: [m() for m in now] and None)
        body(topo, *done, *work_in, *work_out, *work_scr)
        if n_move:
            @pl.when(step == steps - 1)
            def _():
                for d, m in due:
                    if d >= steps:
                        m()
                ex.drain()

    return pl.pallas_call(kernel, grid=grid, out_shape=tuple(outs), in_specs=in_specs, out_specs=tuple(out_specs),
                          scratch_shapes=scratch + sems, compiler_params=pltpu.CompilerParams(**compiler), name=name)(*ins)


def project(sh, params, z, m, **move):
    return call(sh, "project", _project_kernel, sh.grid, params, (z, m), [sh.z_spec, sh.m_spec],
                [sh.sides], [sh.sides_spec], [sh.scr], **move)


def finish_project(sh, params, z, m, t, **move):
    return call(sh, "finish_project", _finish_project_kernel, sh.grid, params, (z, m, t[0]) + (t[1],) * sh.topo.nb,
                [sh.z_spec, sh.m_spec] + sh.tri_pieces(), [sh.zt, sh.sides], [sh.zt_spec, sh.sides_spec], [sh.scr_y, sh.scr], **move)


def finish(sh, params, zt, t, **move):
    return call(sh, "finish", _finish_kernel, sh.grid, params, (zt, t[0]) + (t[1],) * sh.topo.nb,
                [sh.zt_spec] + sh.tri_pieces(), [sh.z_out], [sh.z_spec], [sh.scr_y], **move)


def finish_last(sh, params, zt, t, other):
    return call(sh, "finish_last", _finish_last_kernel, sh.grid, params, (zt, other, t[0]) + (t[1],) * sh.topo.nb,
                [sh.zt_spec, sh.z_spec] + sh.tri_pieces(), [sh.z_out, sh.z_out], [sh.z_spec, sh.z_spec], [sh.scr_y])


def triangle(sh, sides, contract, **move):
    nb = sh.topo.nb
    return call(sh, "triangle", lambda topo, *refs: _triangle_kernel(topo, contract, *refs), (sh.topo.nq,), (),
                ((sides[0],) + (sides[1],) * nb) * 2, sh.side_pieces(0) + sh.side_pieces(1),
                [sh.tri], [pl.BlockSpec((1, None) + sh.bits + (sh.rows, sh.width), lambda q: (q,) + (0,) * (nb + 3))],
                [sh.mat, sh.mat], **move)


def solution(mesh):
    n = mesh.shape["dap"]
    row_spec = P(("data", "dap"), None, None)
    mask_spec = P(("data", "dap"), None)
    rep = P()

    def per_device(z_one, mask_one, z_two, mask_two, norm_in, w_proj, w_gate, norm_mid, w_out):
        sh = Shapes(n, z_one, w_proj)
        first = ((norm_in, 0), (w_proj, 0))
        middle = ((norm_in, 0), (norm_mid, 0), (w_gate, 0), (w_out, 0), (norm_in, 1), (w_proj, 1))
        last = ((norm_in, 1), (norm_mid, 1), (w_gate, 1), (w_out, 1))
        s1, = project(sh, first, z_one, mask_one)
        s2, w1 = project(sh, first, z_two, mask_two, moving=s1, cid=0, pace=6)
        t1, w2 = triangle(sh, (s1, w1), 1, moving=s2, cid=1)
        t2, v1 = triangle(sh, (s2, w2), 1, moving=t1, cid=2)
        zt1, s1, v2 = finish_project(sh, middle, z_one, mask_one, (t1, v1), moving=t2, cid=3, pace=1.6)
        zt2, s2, w1 = finish_project(sh, middle, z_two, mask_two, (t2, v2), moving=s1, cid=4, pace=3.2)
        t1, w2 = triangle(sh, (s1, w1), 0, moving=s2, cid=5)
        t2, v1 = triangle(sh, (s2, w2), 0, moving=t1, cid=6)
        z1, v2 = finish(sh, last, zt1, (t1, v1), moving=t2, cid=7, pace=3.4)
        z2, z1 = finish_last(sh, last, zt2, (t2, v2), z1)
        return z1, z2

    return jax.shard_map(per_device, mesh=mesh,
                         in_specs=(row_spec, mask_spec, row_spec, mask_spec, rep, rep, rep, rep, rep),
                         out_specs=(row_spec, row_spec), check_vma=False)
```

```python
import functools
import math

import jax
import jax.numpy as jnp
from jax import lax
from jax.experimental import pallas as pl
from jax.experimental.pallas import tpu as pltpu
from jax.sharding import PartitionSpec as P

RB = 8
LANES = 128
PART = 128
F32, BF16 = jnp.float32, jnp.bfloat16


def _norm_cols(v, gain, shift):
    mean = jnp.mean(v, axis=0, keepdims=True)
    cen = v - mean
    var = jnp.mean(cen * cen, axis=0, keepdims=True)
    return (cen * lax.rsqrt(var + 1e-5) * gain + shift).astype(BF16)


def _mm(a, b):
    return lax.dot_general(a, b, (((1,), (0,)), ((), ())), preferred_element_type=F32)


def _project(zs, norm_ref, wp_ref, scr, r):
    hid = wp_ref.shape[0] // 4
    x = jnp.concatenate([_norm_cols(z_t, norm_ref[0], norm_ref[1]) for z_t in zs], axis=1)
    part = min(PART, hid)
    for s in range(2):
        for h in range(0, hid, part):
            p = _mm(wp_ref[2 * s * hid + h:2 * s * hid + h + part], x)
            g = _mm(wp_ref[(2 * s + 1) * hid + h:(2 * s + 1) * hid + h + part], x)
            for kk in range(len(zs)):
                lanes = slice(kk * LANES, (kk + 1) * LANES)
                v = jax.nn.sigmoid(g[:, lanes]) * p[:, lanes]
                scr[kk, pl.ds((s * hid + h) * RB + r, part, stride=RB), :] = v


def _each_tile(width, f):
    def body(kk, c):
        f(kk, pl.ds(pl.multiple_of(kk * LANES, LANES), LANES))
        return c
    lax.fori_loop(0, width // LANES, body, 0)


def _emit_sides(scr, m_ref, out_ref, topo):
    half = scr.shape[1] // 2

    def tile(kk, lanes):
        keep = m_ref[:, lanes].astype(F32)
        for q in range(topo.nq):
            for s in range(2):
                for rho, owner in topo.blocks(topo.order(q)):
                    at = pl.multiple_of(s * half + (owner * topo.nq + q) * RB, RB)
                    out_ref[(q, s) + rho + (slice(None), lanes)] = (scr[kk, pl.ds(at, RB), :] * keep).astype(BF16)
    _each_tile(m_ref.shape[1], tile)


def _finish(z_t, r, kk, scr_y, norm_ref, mid_ref, wg_ref, wo_ref):
    hid = wo_ref.shape[1]
    gate = jax.nn.sigmoid(_mm(wg_ref[...], _norm_cols(z_t, norm_ref[0], norm_ref[1])))
    y = scr_y[kk, pl.ds(r, hid, stride=RB), :]
    y = (y * mid_ref[0] + mid_ref[1]).astype(BF16)
    return (z_t + gate * _mm(wo_ref[...], y)).astype(BF16)


def _norm_mid(t_refs, scr_y, topo):
    tiles = [(q,) + rest for q in range(topo.nq) for rest in topo.landed(topo.order(q))]
    inv_n = 1.0 / len(tiles)

    def tile(kk, lanes):
        def load(t):
            return t_refs[t[1]][(t[0],) + t[2] + (slice(None), lanes)].astype(F32)

        def total(f):
            part = [f(load(t)) for t in tiles[:4]]
            for i, t in enumerate(tiles[4:]):
                part[i % 4] = part[i % 4] + f(load(t))
            return (part[0] + part[1]) + (part[2] + part[3])
        mean = total(lambda v: v) * inv_n
        inv = lax.rsqrt(total(lambda v: (v - mean) * (v - mean)) * inv_n + 1e-5)
        for t in tiles:
            at = pl.multiple_of((t[3] * topo.nq + t[0]) * RB, RB)
            scr_y[kk, pl.ds(at, RB), :] = (load(t) - mean) * inv
    _each_tile(scr_y.shape[0] * LANES, tile)


def _lanes(width):
    return [slice(at, at + LANES) for at in range(0, width, LANES)]


def _row_loop(f, unroll=RB):
    def body(i, c):
        for u in range(unroll):
            f(i * unroll + u)
        return c
    lax.fori_loop(0, RB // unroll, body, 0)


class Topo:
    def __init__(self, n):
        self.side = math.isqrt(n // 2)
        ring = self.side.bit_length() - 1
        self.nq = 2 * ring
        self.nb = self.nq + 1
        self.links = [(axis, bit) for bit in range(ring) for axis in ("x", "y")]
        self.weight = {("core", 0): 1}
        self.weight.update({("x", b): 2 << b for b in range(ring)})
        self.weight.update({("y", b): (2 << ring) << b for b in range(ring)})

    def order(self, q):
        links = [self.links[(q + i) % self.nq] for i in range(self.nq)]
        return links[:self.nq // 2] + [("core", 0)] + links[self.nq // 2:]

    def here(self):
        me = lax.axis_index("dap")
        self.pos = {"core": lax.rem(me, 2), "x": lax.rem(me // 2, self.side), "y": me // (2 * self.side)}
        self.bit = {}
        for axis, b in self.weight:
            v = self.pos[axis]
            self.bit[axis, b] = lax.rem(v // (1 << b) + v // (2 << b), 2) if axis != "core" else v
        return self

    def neighbour(self, link):
        axis, b = link
        pos = dict(self.pos)
        v, span = pos[axis], 2 << b
        pos[axis] = v - lax.rem(v, span) + (span - 1) - lax.rem(v, span)
        return (pos["y"] * self.side + pos["x"]) * 2 + pos["core"]

    def partner(self, q, s):
        if s == self.nq // 2:
            return self.neighbour(("core", 0))
        at = s if s < self.nq // 2 else s - 1
        i = lax.rem(q + at, self.nq)
        hit = [jnp.where(i == k, self.neighbour(link), 0) for k, link in enumerate(self.links)]
        return functools.reduce(lambda u, v: u + v, hit)

    def blocks(self, order):
        out = [((), 0)]
        for link in order:
            w, own = self.weight[link], self.bit[link]
            out = [(r + (f,), o + w * (1 - own if f else own)) for r, o in out for f in (0, 1)]
        return out

    def landed(self, order):
        out = []
        for rho, owner in self.blocks(order):
            last = max([i for i, f in enumerate(rho) if f], default=-1)
            idx = (0,) * self.nb if last < 0 else rho[:last] + (0,) * (self.nb - last)
            out.append((last + 1, idx, owner))
        return out

    def natural(self, owner):
        side, core, rest = self.side, lax.rem(owner, 2), owner // 2
        gx, gy = lax.rem(rest, side), rest // side

        def binary(g):
            v, b = 0, 0
            k = side.bit_length() - 2
            for i in range(k, -1, -1):
                b = lax.rem(b + lax.rem(g // (1 << i), 2), 2)
                v = v + b * (1 << i)
            return v
        return (binary(gy) * side + binary(gx)) * 2 + core

    def gray_bits(self, p):
        pos = {"core": p % 2, "x": p // 2 % self.side, "y": p // 2 // self.side}
        return {k: (pos[k[0]] if k[0] == "core" else (pos[k[0]] >> k[1] ^ pos[k[0]] >> (k[1] + 1)) & 1) for k in self.weight}

    def relative(self, order, p):
        bits = self.gray_bits(p)
        return tuple((1 - self.bit[k]) if bits[k] else self.bit[k] for k in order)


class Exchange:
    def __init__(self, topo, src, dst, ssem, rsem):
        self.topo, self.src, self.dst, self.ssem, self.rsem = topo, src, dst, ssem, rsem
        self.cut = src.shape[1] == 1

    def _tail(self, sub):
        if not self.cut:
            return sub, ()
        w = self.src.shape[-1] // 2
        return 0, (slice(None), pl.ds(sub * w, w))

    def _copy(self, q, sub, s, a, b):
        return pltpu.make_async_remote_copy(
            src_ref=a, dst_ref=b, send_sem=self.ssem.at[q, sub, s], recv_sem=self.rsem.at[q, sub, s],
            device_id={"dap": self.topo.partner(q, s)}, device_id_type=pl.DeviceIdType.MESH)

    def _streams(self, f):
        def body(q, c):
            f(q)
            return c
        lax.fori_loop(0, self.topo.nq, body, 0)

    def start(self, sub, s):
        nb, free = self.topo.nb, (slice(None),)
        k, tail = self._tail(sub)

        def stream(q):
            for t in range(-1, s):
                if t < 0:
                    idx = (0,) * s + (1,) + free * (nb - 1 - s) + tail
                    a = self.src.at[(q, k) + idx]
                else:
                    idx = free * t + (1,) + (0,) * (s - 1 - t) + (1,) + free * (nb - 1 - s) + tail
                    a = self.dst.at[(q, k, t) + idx]
                self._copy(q, sub, s, a, self.dst.at[(q, k, s) + idx]).start()
        self._streams(stream)

    def _whole(self, q, sub, s):
        k, tail = self._tail(sub)
        ref = self.dst.at[(q, k, s) + (slice(None),) * s + (1,) + (slice(None),) * (self.topo.nb - 1 - s) + tail]
        return self._copy(q, sub, s, ref, ref)

    def arrive(self, sub, s):
        self._streams(lambda q: self._whole(q, sub, s).wait_recv())

    def drain(self):
        for sub in range(2):
            for s in range(self.topo.nb):
                self._streams(lambda q, sub=sub, s=s: self._whole(q, sub, s).wait_send())

    def barrier(self):
        bar = pltpu.get_barrier_semaphore()
        for link in self.topo.weight:
            pl.semaphore_signal(bar, inc=1, device_id={"dap": self.topo.neighbour(link)}, device_id_type=pl.DeviceIdType.MESH)
        pl.semaphore_wait(bar, len(self.topo.weight))

    def moves(self):
        mid, out = self.topo.nq // 2, []
        for s in range(self.topo.nb):
            for sub in range(2):
                def move(s=s, sub=sub):
                    self.arrive(sub, s)
                    if s + 1 < self.topo.nb:
                        self.start(sub, s + 1)
                out.append((2 * s + sub + 1 if s < mid else 2 * s + sub - 0.5 if s == mid else 2 * s + sub - 1, move))
        return sorted(out, key=lambda m: m[0])


def _project_kernel(topo, norm, wp, z_ref, m_ref, out_ref, scr):
    _row_loop(lambda r: _project([z_ref[r, lanes, :].T.astype(F32) for lanes in _lanes(z_ref.shape[1])], norm, wp, scr, r))
    _emit_sides(scr, m_ref, out_ref, topo)


def _finish_project_kernel(topo, n0, mid, wg, wo, n1, wp, z_ref, m_ref, *refs):
    t_refs, (zt_ref, out_ref, scr_y, scr) = refs[:-4], refs[-4:]
    _norm_mid(t_refs, scr_y, topo)

    def row(r):
        news = []
        for kk, lanes in enumerate(_lanes(z_ref.shape[1])):
            z_new = _finish(z_ref[r, lanes, :].T.astype(F32), r, kk, scr_y, n0, mid, wg, wo)
            zt_ref[r, :, lanes] = z_new
            news.append(z_new.astype(F32))
        _project(news, n1, wp, scr, r)
    _row_loop(row, RB // 2)
    _emit_sides(scr, m_ref, out_ref, topo)


def _finish_kernel(topo, n0, mid, wg, wo, zt_ref, *refs):
    t_refs, (z_ref, scr_y) = refs[:-2], refs[-2:]
    _norm_mid(t_refs, scr_y, topo)

    def row(r):
        for kk, lanes in enumerate(_lanes(z_ref.shape[1])):
            z_new = _finish(zt_ref[r, :, lanes].astype(F32), r, kk, scr_y, n0, mid, wg, wo)
            z_ref[r, lanes, :] = z_new.T
    _row_loop(row)


def _finish_last_kernel(topo, n0, mid, wg, wo, zt_ref, other_ref, *refs):
    t_refs, (z_ref, other_out, scr_y) = refs[:-3], refs[-3:]
    other_out[...] = other_ref[...]
    _finish_kernel(topo, n0, mid, wg, wo, zt_ref, *t_refs, z_ref, scr_y)


def _triangle_kernel(topo, contract, s_ref, w_ref, out_ref, a_scr, b_scr, t_scr, in_sem, out_sem):
    n, rows, width = a_scr.shape[1:]
    step = pl.program_id(0)
    slot = lax.rem(step, 2)

    def load(q):
        for i, (rho, owner) in enumerate(topo.blocks(topo.order(q))):
            last = max([k for k, f in enumerate(rho) if f], default=-1)
            for side, scr in enumerate((a_scr, b_scr)):
                src = s_ref.at[(q, side) + rho] if last < 0 else w_ref.at[(q, side, last) + rho]
                at = topo.natural(owner) if side and contract else i
                pltpu.make_async_copy(src, scr.at[q % 2, at], in_sem.at[q % 2, side]).start()

    def store(q):
        if contract:
            places = [rho for rho, _ in topo.blocks(topo.order(q))]
        else:
            places = [topo.relative(topo.order(q), p) for p in range(n)]
        for i, place in enumerate(places):
            pltpu.make_async_copy(t_scr.at[q % 2, i], out_ref.at[(q, 0) + place], out_sem.at[q % 2]).start()

    def wait(scr, at, sem):
        pltpu.make_async_copy(scr.at[at], scr.at[at], sem).wait()

    for q in range(topo.nq):
        @pl.when(step == q)
        def _():
            if q == 0:
                load(0)
            if q + 1 < topo.nq:
                load(q + 1)
    wait(a_scr, slot, in_sem.at[slot, 0])
    wait(b_scr, slot, in_sem.at[slot, 1])
    a, b = a_scr[slot].reshape(n * rows, width), b_scr[slot].reshape(n * rows, width)
    t = lax.dot_general(a, b, (((contract,), (contract,)), ((), ())), preferred_element_type=F32)

    @pl.when(step >= 2)
    def _():
        wait(t_scr, slot, out_sem.at[slot])
    t_scr[slot] = t.astype(BF16).reshape(n, rows, width)
    for q in range(topo.nq):
        pl.when(step == q)(functools.partial(store, q))

    @pl.when(step == topo.nq - 1)
    def _():
        for k in range(min(2, topo.nq)):
            wait(t_scr, k, out_sem.at[k])


def _whole(a):
    return pl.BlockSpec(a.shape, lambda *_: (0,) * a.ndim)


class Shapes:
    def __init__(self, n, z, w_proj):
        self.topo = topo = Topo(n)
        self.n, (self.rows, self.width, self.cz) = n, z.shape
        self.hid = w_proj.shape[-1] // 4
        assert self.hid == n * topo.nq
        self.kb = 2 * LANES if self.width % (2 * LANES) == 0 else LANES
        self.grid = (self.rows // RB, self.width // self.kb)
        self.bits = (2,) * topo.nb
        zero = (0,) * topo.nb
        self.z_spec = pl.BlockSpec((RB, self.kb, self.cz), lambda i, j: (i, j, 0))
        self.zt_spec = pl.BlockSpec((RB, self.cz, self.kb), lambda i, j: (i, 0, j))
        self.m_spec = pl.BlockSpec((RB, self.kb), lambda i, j: (i, j))
        self.sides_spec = pl.BlockSpec((topo.nq, 2) + self.bits + (RB, self.kb), lambda i, j: (0, 0) + zero + (i, j))
        self.sides = jax.ShapeDtypeStruct((topo.nq, 2) + self.bits + (self.rows, self.width), BF16)
        self.tri = jax.ShapeDtypeStruct((topo.nq, 1) + self.bits + (self.rows, self.width), BF16)
        self.z_out = jax.ShapeDtypeStruct(z.shape, BF16)
        self.zt = jax.ShapeDtypeStruct((self.rows, self.cz, self.width), BF16)
        self.scr = pltpu.VMEM((self.kb // LANES, 2 * self.hid * RB, LANES), F32)
        self.scr_y = pltpu.VMEM((self.kb // LANES, self.hid * RB, LANES), F32)
        self.mat = pltpu.VMEM((2, n, self.rows, self.width), BF16)

    def landing(self, src):
        return jax.ShapeDtypeStruct(src.shape[:2] + (self.topo.nb,) + src.shape[2:], BF16)

    def _pieces(self, head, tail, index):
        nb = self.topo.nb
        specs = [pl.BlockSpec((head, None) + (1,) * nb + tail, lambda *g: index(g)[0] + (0,) * nb + index(g)[1])]
        for s in range(nb):
            at = (0,) * s + (1,) + (0,) * (nb - 1 - s)
            specs.append(pl.BlockSpec((head, None, None) + (2,) * s + (1,) * (nb - s) + tail,
                                      lambda *g, s=s, at=at: index(g)[0] + (s,) + at + index(g)[1]))
        return specs

    def tri_pieces(self):
        return self._pieces(self.topo.nq, (RB, self.kb), lambda g: ((0, 0), (g[0], g[1])))


def _prepare(raw, ready, update):
    if len(ready.shape) == 3:
        for i in range(2):
            row = raw[update, i:i + 1, :].astype(F32)
            ready[i] = jnp.broadcast_to(row, (LANES, row.shape[1])).T
    else:
        ready[...] = raw[update].astype(F32).T.astype(BF16)


def call(sh, name, body, grid, params, ins, in_specs, outs, out_specs, scratch, moving=None, cid=0, pace=None):
    topo = sh.topo
    steps = math.prod(grid)
    compiler = dict(vmem_limit_bytes=62 * 1024 * 1024)
    hbm = pl.BlockSpec(memory_space=pl.ANY)
    n_par, n_in, n_out = len(params), len(ins), len(outs)
    ready = [pltpu.VMEM((2, p.shape[-1], LANES), F32) if p.shape[1] == 2 else pltpu.VMEM(p.shape[:0:-1], BF16) for p, _ in params]
    ins, in_specs = [p for p, _ in params] + list(ins), [_whole(p) for p, _ in params] + list(in_specs)
    scratch, sems = ready + list(scratch), []
    if moving is not None:
        ins, in_specs = ins + [moving], in_specs + [hbm]
        outs, out_specs = list(outs) + [sh.landing(moving)], list(out_specs) + [hbm]
        sems = [pltpu.SemaphoreType.DMA((topo.nq, 2, topo.nb))] * 2
        compiler.update(collective_id=cid, has_side_effects=True)
    n_move = len(sems) // 2

    def kernel(*refs):
        topo.here()
        raw, refs = refs[:n_par], refs[n_par:]
        work_in, refs = refs[:n_in], refs[n_in:]
        src, refs = refs[:n_move], refs[n_move:]
        work_out, refs = refs[:n_out], refs[n_out:]
        dst, refs = refs[:n_move], refs[n_move:]
        done, work_scr, sem_refs = refs[:n_par], refs[n_par:len(refs) - 2 * n_move], refs[len(refs) - 2 * n_move:]
        step = pl.program_id(0)
        for d, size in enumerate(grid[1:], 1):
            step = step * size + pl.program_id(d)
        due = []
        if n_move:
            ex = Exchange(topo, src[0], dst[0], *sem_refs)
            due = [(max(1, round(t * pace)) if pace else steps, m) for t, m in ex.moves()]

        @pl.when(step == 0)
        def _():
            if n_move:
                ex.barrier()
                for sub in range(2):
                    ex.start(sub, 0)
            for a, b, (_, update) in zip(raw, done, params):
                _prepare(a, b, update)
        for g in range(1, steps):
            now = [m for d, m in due if d == g]
            if now:
                pl.when(step == g)(lambda now=now: [m() for m in now] and None)
        body(topo, *done, *work_in, *work_out, *work_scr)
        if n_move:
            @pl.when(step == steps - 1)
            def _():
                for d, m in due:
                    if d >= steps:
                        m()
                ex.drain()

    return pl.pallas_call(kernel, grid=grid, out_shape=tuple(outs), in_specs=in_specs, out_specs=tuple(out_specs),
                          scratch_shapes=scratch + sems, compiler_params=pltpu.CompilerParams(**compiler), name=name)(*ins)


def project(sh, params, z, m, **move):
    return call(sh, "project", _project_kernel, sh.grid, params, (z, m), [sh.z_spec, sh.m_spec],
                [sh.sides], [sh.sides_spec], [sh.scr], **move)


def finish_project(sh, params, z, m, t, **move):
    return call(sh, "finish_project", _finish_project_kernel, sh.grid, params, (z, m, t[0]) + (t[1],) * sh.topo.nb,
                [sh.z_spec, sh.m_spec] + sh.tri_pieces(), [sh.zt, sh.sides], [sh.zt_spec, sh.sides_spec], [sh.scr_y, sh.scr], **move)


def finish(sh, params, zt, t, **move):
    return call(sh, "finish", _finish_kernel, sh.grid, params, (zt, t[0]) + (t[1],) * sh.topo.nb,
                [sh.zt_spec] + sh.tri_pieces(), [sh.z_out], [sh.z_spec], [sh.scr_y], **move)


def finish_last(sh, params, zt, t, other):
    return call(sh, "finish_last", _finish_last_kernel, sh.grid, params, (zt, other, t[0]) + (t[1],) * sh.topo.nb,
                [sh.zt_spec, sh.z_spec] + sh.tri_pieces(), [sh.z_out, sh.z_out], [sh.z_spec, sh.z_spec], [sh.scr_y])


def triangle(sh, sides, contract, **move):
    hbm = pl.BlockSpec(memory_space=pl.ANY)
    return call(sh, "triangle", lambda topo, *refs: _triangle_kernel(topo, contract, *refs), (sh.topo.nq,), (),
                sides, [hbm, hbm], [sh.tri], [hbm],
                [sh.mat, sh.mat, sh.mat, pltpu.SemaphoreType.DMA((2, 2)), pltpu.SemaphoreType.DMA((2,))], **move)


def solution(mesh):
    n = mesh.shape["dap"]
    row_spec = P(("data", "dap"), None, None)
    mask_spec = P(("data", "dap"), None)
    rep = P()

    def per_device(z_one, mask_one, z_two, mask_two, norm_in, w_proj, w_gate, norm_mid, w_out):
        sh = Shapes(n, z_one, w_proj)
        first = ((norm_in, 0), (w_proj, 0))
        middle = ((norm_in, 0), (norm_mid, 0), (w_gate, 0), (w_out, 0), (norm_in, 1), (w_proj, 1))
        last = ((norm_in, 1), (norm_mid, 1), (w_gate, 1), (w_out, 1))
        s1, = project(sh, first, z_one, mask_one)
        s2, w1 = project(sh, first, z_two, mask_two, moving=s1, cid=0, pace=6)
        t1, w2 = triangle(sh, (s1, w1), 1, moving=s2, cid=1)
        t2, v1 = triangle(sh, (s2, w2), 1, moving=t1, cid=2)
        zt1, s1, v2 = finish_project(sh, middle, z_one, mask_one, (t1, v1), moving=t2, cid=3, pace=1.3)
        zt2, s2, w1 = finish_project(sh, middle, z_two, mask_two, (t2, v2), moving=s1, cid=4, pace=3.2)
        t1, w2 = triangle(sh, (s1, w1), 0, moving=s2, cid=5)
        t2, v1 = triangle(sh, (s2, w2), 0, moving=t1, cid=6)
        z1, v2 = finish(sh, last, zt1, (t1, v1), moving=t2, cid=7, pace=3.4)
        z2, z1 = finish_last(sh, last, zt2, (t2, v2), z1)
        return z1, z2

    return jax.shard_map(per_device, mesh=mesh,
                         in_specs=(row_spec, mask_spec, row_spec, mask_spec, rep, rep, rep, rep, rep),
                         out_specs=(row_spec, row_spec), check_vma=False)
```

```python
import functools
import math

import jax
import jax.numpy as jnp
from jax import lax
from jax.experimental import pallas as pl
from jax.experimental.pallas import tpu as pltpu
from jax.sharding import PartitionSpec as P

RB = 8
LANES = 128
PART = 128
F32, BF16 = jnp.float32, jnp.bfloat16


def _norm_cols(v, gain, shift):
    mean = jnp.mean(v, axis=0, keepdims=True)
    cen = v - mean
    var = jnp.mean(cen * cen, axis=0, keepdims=True)
    return (cen * lax.rsqrt(var + 1e-5) * gain + shift).astype(BF16)


def _mm(a, b):
    return lax.dot_general(a, b, (((1,), (0,)), ((), ())), preferred_element_type=F32)


def _project(zs, norm_ref, wp_ref, scr, r):
    hid = wp_ref.shape[0] // 4
    x = jnp.concatenate([_norm_cols(z_t, norm_ref[0], norm_ref[1]) for z_t in zs], axis=1)
    part = min(PART, hid)
    for s in range(2):
        for h in range(0, hid, part):
            p = _mm(wp_ref[2 * s * hid + h:2 * s * hid + h + part], x)
            g = _mm(wp_ref[(2 * s + 1) * hid + h:(2 * s + 1) * hid + h + part], x)
            for kk in range(len(zs)):
                lanes = slice(kk * LANES, (kk + 1) * LANES)
                v = jax.nn.sigmoid(g[:, lanes]) * p[:, lanes]
                scr[kk, pl.ds((s * hid + h) * RB + r, part, stride=RB), :] = v


def _each_tile(width, f):
    def body(kk, c):
        f(kk, pl.ds(pl.multiple_of(kk * LANES, LANES), LANES))
        return c
    lax.fori_loop(0, width // LANES, body, 0)


def _emit_sides(scr, m_ref, out_ref, topo):
    half = scr.shape[1] // 2

    def tile(kk, lanes):
        keep = m_ref[:, lanes].astype(F32)
        for q in range(topo.nq):
            for s in range(2):
                for rho, owner in topo.blocks(topo.order(q)):
                    at = pl.multiple_of(s * half + (owner * topo.nq + q) * RB, RB)
                    out_ref[(q, s) + rho + (slice(None), lanes)] = (scr[kk, pl.ds(at, RB), :] * keep).astype(BF16)
    _each_tile(m_ref.shape[1], tile)


def _finish(z_t, r, kk, scr_y, norm_ref, mid_ref, wg_ref, wo_ref):
    hid = wo_ref.shape[1]
    gate = jax.nn.sigmoid(_mm(wg_ref[...], _norm_cols(z_t, norm_ref[0], norm_ref[1])))
    y = scr_y[kk, pl.ds(r, hid, stride=RB), :]
    y = (y * mid_ref[0] + mid_ref[1]).astype(BF16)
    return (z_t + gate * _mm(wo_ref[...], y)).astype(BF16)


def _norm_mid(t_refs, scr_y, topo):
    tiles = [(q,) + rest for q in range(topo.nq) for rest in topo.landed(topo.order(q))]
    inv_n = 1.0 / len(tiles)

    def tile(kk, lanes):
        def load(t):
            return t_refs[t[1]][(t[0],) + t[2] + (slice(None), lanes)].astype(F32)

        def total(f):
            part = [f(load(t)) for t in tiles[:4]]
            for i, t in enumerate(tiles[4:]):
                part[i % 4] = part[i % 4] + f(load(t))
            return (part[0] + part[1]) + (part[2] + part[3])
        mean = total(lambda v: v) * inv_n
        inv = lax.rsqrt(total(lambda v: (v - mean) * (v - mean)) * inv_n + 1e-5)
        for t in tiles:
            at = pl.multiple_of((t[3] * topo.nq + t[0]) * RB, RB)
            scr_y[kk, pl.ds(at, RB), :] = (load(t) - mean) * inv
    _each_tile(scr_y.shape[0] * LANES, tile)


def _lanes(width):
    return [slice(at, at + LANES) for at in range(0, width, LANES)]


def _row_loop(f, unroll=RB):
    def body(i, c):
        for u in range(unroll):
            f(i * unroll + u)
        return c
    lax.fori_loop(0, RB // unroll, body, 0)


class Topo:
    def __init__(self, n):
        self.side = math.isqrt(n // 2)
        ring = self.side.bit_length() - 1
        self.nq = 2 * ring
        self.nb = self.nq + 1
        self.links = [(axis, bit) for bit in range(ring) for axis in ("x", "y")]
        self.weight = {("core", 0): 1}
        self.weight.update({("x", b): 2 << b for b in range(ring)})
        self.weight.update({("y", b): (2 << ring) << b for b in range(ring)})

    def order(self, q):
        links = [self.links[(q + i) % self.nq] for i in range(self.nq)]
        return links[:self.nq // 2] + [("core", 0)] + links[self.nq // 2:]

    def here(self):
        me = lax.axis_index("dap")
        self.pos = {"core": lax.rem(me, 2), "x": lax.rem(me // 2, self.side), "y": me // (2 * self.side)}
        self.bit = {}
        for axis, b in self.weight:
            v = self.pos[axis]
            self.bit[axis, b] = lax.rem(v // (1 << b) + v // (2 << b), 2) if axis != "core" else v
        return self

    def neighbour(self, link):
        axis, b = link
        pos = dict(self.pos)
        v, span = pos[axis], 2 << b
        pos[axis] = v - lax.rem(v, span) + (span - 1) - lax.rem(v, span)
        return (pos["y"] * self.side + pos["x"]) * 2 + pos["core"]

    def partner(self, q, s):
        if s == self.nq // 2:
            return self.neighbour(("core", 0))
        at = s if s < self.nq // 2 else s - 1
        i = lax.rem(q + at, self.nq)
        hit = [jnp.where(i == k, self.neighbour(link), 0) for k, link in enumerate(self.links)]
        return functools.reduce(lambda u, v: u + v, hit)

    def blocks(self, order):
        out = [((), 0)]
        for link in order:
            w, own = self.weight[link], self.bit[link]
            out = [(r + (f,), o + w * (1 - own if f else own)) for r, o in out for f in (0, 1)]
        return out

    def landed(self, order):
        out = []
        for rho, owner in self.blocks(order):
            last = max([i for i, f in enumerate(rho) if f], default=-1)
            idx = (0,) * self.nb if last < 0 else rho[:last] + (0,) * (self.nb - last)
            out.append((last + 1, idx, owner))
        return out

    def natural(self, owner):
        side, core, rest = self.side, lax.rem(owner, 2), owner // 2
        gx, gy = lax.rem(rest, side), rest // side

        def binary(g):
            v, b = 0, 0
            k = side.bit_length() - 2
            for i in range(k, -1, -1):
                b = lax.rem(b + lax.rem(g // (1 << i), 2), 2)
                v = v + b * (1 << i)
            return v
        return (binary(gy) * side + binary(gx)) * 2 + core

    def gray_bits(self, p):
        pos = {"core": p % 2, "x": p // 2 % self.side, "y": p // 2 // self.side}
        return {k: (pos[k[0]] if k[0] == "core" else (pos[k[0]] >> k[1] ^ pos[k[0]] >> (k[1] + 1)) & 1) for k in self.weight}

    def relative(self, order, p):
        bits = self.gray_bits(p)
        return tuple((1 - self.bit[k]) if bits[k] else self.bit[k] for k in order)


class Exchange:
    def __init__(self, topo, src, dst, ssem, rsem):
        self.topo, self.src, self.dst, self.ssem, self.rsem = topo, src, dst, ssem, rsem
        self.cut = src.shape[1] == 1

    def _tail(self, sub):
        if not self.cut:
            return sub, ()
        w = self.src.shape[-1] // 2
        return 0, (slice(None), pl.ds(sub * w, w))

    def _copy(self, q, sub, s, a, b):
        return pltpu.make_async_remote_copy(
            src_ref=a, dst_ref=b, send_sem=self.ssem.at[q, sub, s], recv_sem=self.rsem.at[q, sub, s],
            device_id={"dap": self.topo.partner(q, s)}, device_id_type=pl.DeviceIdType.MESH)

    def _streams(self, f):
        def body(q, c):
            f(q)
            return c
        lax.fori_loop(0, self.topo.nq, body, 0)

    def start(self, sub, s):
        nb, free = self.topo.nb, (slice(None),)
        k, tail = self._tail(sub)

        def stream(q):
            for t in range(-1, s):
                if t < 0:
                    idx = (0,) * s + (1,) + free * (nb - 1 - s) + tail
                    a = self.src.at[(q, k) + idx]
                else:
                    idx = free * t + (1,) + (0,) * (s - 1 - t) + (1,) + free * (nb - 1 - s) + tail
                    a = self.dst.at[(q, k, t) + idx]
                self._copy(q, sub, s, a, self.dst.at[(q, k, s) + idx]).start()
        self._streams(stream)

    def _whole(self, q, sub, s):
        k, tail = self._tail(sub)
        ref = self.dst.at[(q, k, s) + (slice(None),) * s + (1,) + (slice(None),) * (self.topo.nb - 1 - s) + tail]
        return self._copy(q, sub, s, ref, ref)

    def arrive(self, sub, s):
        self._streams(lambda q: self._whole(q, sub, s).wait_recv())

    def drain(self):
        for sub in range(2):
            for s in range(self.topo.nb):
                self._streams(lambda q, sub=sub, s=s: self._whole(q, sub, s).wait_send())

    def barrier(self):
        bar = pltpu.get_barrier_semaphore()
        for link in self.topo.weight:
            pl.semaphore_signal(bar, inc=1, device_id={"dap": self.topo.neighbour(link)}, device_id_type=pl.DeviceIdType.MESH)
        pl.semaphore_wait(bar, len(self.topo.weight))

    def moves(self):
        mid, out = self.topo.nq // 2, []
        for s in range(self.topo.nb):
            for sub in range(2):
                def move(s=s, sub=sub):
                    self.arrive(sub, s)
                    if s + 1 < self.topo.nb:
                        self.start(sub, s + 1)
                out.append((2 * s + sub + 1 if s < mid else 2 * s + sub - 0.5 if s == mid else 2 * s + sub - 1, move))
        return sorted(out, key=lambda m: m[0])


def _project_kernel(topo, norm, wp, z_ref, m_ref, out_ref, scr):
    _row_loop(lambda r: _project([z_ref[r, lanes, :].T.astype(F32) for lanes in _lanes(z_ref.shape[1])], norm, wp, scr, r))
    _emit_sides(scr, m_ref, out_ref, topo)


def _finish_project_kernel(topo, n0, mid, wg, wo, n1, wp, z_ref, m_ref, *refs):
    t_refs, (zt_ref, out_ref, scr_y, scr) = refs[:-4], refs[-4:]
    _norm_mid(t_refs, scr_y, topo)

    def row(r):
        news = []
        for kk, lanes in enumerate(_lanes(z_ref.shape[1])):
            z_new = _finish(z_ref[r, lanes, :].T.astype(F32), r, kk, scr_y, n0, mid, wg, wo)
            zt_ref[r, :, lanes] = z_new
            news.append(z_new.astype(F32))
        _project(news, n1, wp, scr, r)
    _row_loop(row, RB // 2)
    _emit_sides(scr, m_ref, out_ref, topo)


def _finish_kernel(topo, n0, mid, wg, wo, zt_ref, *refs):
    t_refs, (z_ref, scr_y) = refs[:-2], refs[-2:]
    _norm_mid(t_refs, scr_y, topo)

    def row(r):
        for kk, lanes in enumerate(_lanes(z_ref.shape[1])):
            z_new = _finish(zt_ref[r, :, lanes].astype(F32), r, kk, scr_y, n0, mid, wg, wo)
            z_ref[r, lanes, :] = z_new.T
    _row_loop(row)


def _finish_last_kernel(topo, n0, mid, wg, wo, zt_ref, other_ref, *refs):
    t_refs, (z_ref, other_out, scr_y) = refs[:-3], refs[-3:]
    other_out[...] = other_ref[...]
    _finish_kernel(topo, n0, mid, wg, wo, zt_ref, *t_refs, z_ref, scr_y)


def _triangle_kernel(topo, contract, s_ref, w_ref, out_ref, a_scr, b_scr, t_scr, in_sem, out_sem):
    n, rows, width = a_scr.shape[1:]
    step = pl.program_id(0)
    slot = lax.rem(step, 2)

    def load(q):
        for i, (rho, owner) in enumerate(topo.blocks(topo.order(q))):
            last = max([k for k, f in enumerate(rho) if f], default=-1)
            for side, scr in enumerate((a_scr, b_scr)):
                src = s_ref.at[(q, side) + rho] if last < 0 else w_ref.at[(q, side, last) + rho]
                at = topo.natural(owner) if side and contract else i
                pltpu.make_async_copy(src, scr.at[q % 2, at], in_sem.at[q % 2, side]).start()

    def store(q):
        if contract:
            places = [rho for rho, _ in topo.blocks(topo.order(q))]
        else:
            places = [topo.relative(topo.order(q), p) for p in range(n)]
        for i, place in enumerate(places):
            pltpu.make_async_copy(t_scr.at[q % 2, i], out_ref.at[(q, 0) + place], out_sem.at[q % 2]).start()

    def wait(scr, at, sem):
        pltpu.make_async_copy(scr.at[at], scr.at[at], sem).wait()

    for q in range(topo.nq):
        @pl.when(step == q)
        def _():
            if q == 0:
                load(0)
            if q + 1 < topo.nq:
                load(q + 1)
    wait(a_scr, slot, in_sem.at[slot, 0])
    wait(b_scr, slot, in_sem.at[slot, 1])
    a, b = a_scr[slot].reshape(n * rows, width), b_scr[slot].reshape(n * rows, width)
    t = lax.dot_general(a, b, (((contract,), (contract,)), ((), ())), preferred_element_type=F32)

    @pl.when(step >= 2)
    def _():
        wait(t_scr, slot, out_sem.at[slot])
    t_scr[slot] = t.astype(BF16).reshape(n, rows, width)
    for q in range(topo.nq):
        pl.when(step == q)(functools.partial(store, q))

    @pl.when(step == topo.nq - 1)
    def _():
        for k in range(min(2, topo.nq)):
            wait(t_scr, k, out_sem.at[k])


def _whole(a):
    return pl.BlockSpec(a.shape, lambda *_: (0,) * a.ndim)


class Shapes:
    def __init__(self, n, z, w_proj):
        self.topo = topo = Topo(n)
        self.n, (self.rows, self.width, self.cz) = n, z.shape
        self.hid = w_proj.shape[-1] // 4
        assert self.hid == n * topo.nq
        self.kb = 2 * LANES if self.width % (2 * LANES) == 0 else LANES
        self.grid = (self.rows // RB, self.width // self.kb)
        self.bits = (2,) * topo.nb
        zero = (0,) * topo.nb
        self.z_spec = pl.BlockSpec((RB, self.kb, self.cz), lambda i, j: (i, j, 0))
        self.zt_spec = pl.BlockSpec((RB, self.cz, self.kb), lambda i, j: (i, 0, j))
        self.m_spec = pl.BlockSpec((RB, self.kb), lambda i, j: (i, j))
        self.sides_spec = pl.BlockSpec((topo.nq, 2) + self.bits + (RB, self.kb), lambda i, j: (0, 0) + zero + (i, j))
        self.sides = jax.ShapeDtypeStruct((topo.nq, 2) + self.bits + (self.rows, self.width), BF16)
        self.tri = jax.ShapeDtypeStruct((topo.nq, 1) + self.bits + (self.rows, self.width), BF16)
        self.z_out = jax.ShapeDtypeStruct(z.shape, BF16)
        self.zt = jax.ShapeDtypeStruct((self.rows, self.cz, self.width), BF16)
        self.scr = pltpu.VMEM((self.kb // LANES, 2 * self.hid * RB, LANES), F32)
        self.scr_y = pltpu.VMEM((self.kb // LANES, self.hid * RB, LANES), F32)
        self.mat = pltpu.VMEM((2, n, self.rows, self.width), BF16)

    def landing(self, src):
        return jax.ShapeDtypeStruct(src.shape[:2] + (self.topo.nb,) + src.shape[2:], BF16)

    def _pieces(self, head, tail, index):
        nb = self.topo.nb
        specs = [pl.BlockSpec((head, None) + (1,) * nb + tail, lambda *g: index(g)[0] + (0,) * nb + index(g)[1])]
        for s in range(nb):
            at = (0,) * s + (1,) + (0,) * (nb - 1 - s)
            specs.append(pl.BlockSpec((head, None, None) + (2,) * s + (1,) * (nb - s) + tail,
                                      lambda *g, s=s, at=at: index(g)[0] + (s,) + at + index(g)[1]))
        return specs

    def tri_pieces(self):
        return self._pieces(self.topo.nq, (RB, self.kb), lambda g: ((0, 0), (g[0], g[1])))


def _prepare(raw, ready, update):
    if len(ready.shape) == 3:
        for i in range(2):
            row = raw[update, i:i + 1, :].astype(F32)
            ready[i] = jnp.broadcast_to(row, (LANES, row.shape[1])).T
    else:
        ready[...] = raw[update].astype(F32).T.astype(BF16)


def _at(ref, spec, grid, g):
    ids = []
    for size in grid[::-1]:
        ids.append(lax.rem(g, size))
        g = g // size
    idx = spec.index_map(*ids[::-1])
    return ref.at[tuple(i if b is None else pl.ds(i * b if isinstance(i, int) else pl.multiple_of(i * b, b), b)
                        for i, b in zip(idx, spec.block_shape))]


def call(sh, name, body, grid, params, ins, in_specs, outs, out_specs, scratch, moving=None, cid=0, pace=None):
    topo = sh.topo
    steps = math.prod(grid)
    compiler = dict(vmem_limit_bytes=62 * 1024 * 1024)
    hbm = pl.BlockSpec(memory_space=pl.ANY)
    n_par, n_in, n_out = len(params), len(ins), len(outs)
    ready = [pltpu.VMEM((2, p.shape[-1], LANES), F32) if p.shape[1] == 2 else pltpu.VMEM(p.shape[:0:-1], BF16) for p, _ in params]
    ins, in_specs = [p for p, _ in params] + list(ins), [_whole(p) for p, _ in params] + list(in_specs)
    scratch, sems = ready + list(scratch), []
    if moving is not None:
        ins, in_specs = ins + [moving], in_specs + [hbm]
        outs, out_specs = list(outs) + [sh.landing(moving)], list(out_specs) + [hbm]
        sems = [pltpu.SemaphoreType.DMA((topo.nq, 2, topo.nb))] * 2
        compiler.update(collective_id=cid, has_side_effects=True)
    n_move = len(sems) // 2
    own_in, own_out = [], []
    if n_move:
        own_in = [(k, in_specs[n_par + k]) for k in range(n_in) if in_specs[n_par + k].block_shape is not None]
        own_out = [(k, out_specs[k]) for k in range(n_out) if out_specs[k].block_shape is not None]
        in_specs = in_specs[:n_par] + [hbm] * (n_in + 1)
        out_specs = [hbm] * (n_out + 1)
        for arrays, own, skip in ((ins, own_in, n_par), (outs, own_out, 0)):
            scratch += [pltpu.VMEM((2,) + tuple(b for b in spec.block_shape if b is not None), arrays[skip + k].dtype) for k, spec in own]
        if own_in:
            sems = [pltpu.SemaphoreType.DMA((2, len(own_in))), pltpu.SemaphoreType.DMA((2, len(own_out)))] + sems

    def kernel(*refs):
        topo.here()
        raw, refs = refs[:n_par], refs[n_par:]
        work_in, refs = refs[:n_in], refs[n_in:]
        src, refs = refs[:n_move], refs[n_move:]
        work_out, refs = refs[:n_out], refs[n_out:]
        dst, refs = refs[:n_move], refs[n_move:]
        refs, sem_refs = refs[:len(refs) - 2 * n_move], refs[len(refs) - 2 * n_move:]
        if own_in:
            in_sem, out_sem = refs[-2:]
            held = refs[-2 - len(own_in) - len(own_out):-2]
            refs = refs[:-2 - len(own_in) - len(own_out)]
        done, work_scr = refs[:n_par], refs[n_par:]
        step = pl.program_id(0)
        for d, size in enumerate(grid[1:], 1):
            step = step * size + pl.program_id(d)
        due = []
        if n_move:
            ex = Exchange(topo, src[0], dst[0], *sem_refs)
            due = [(max(1, round(t * pace)) if pace else steps, m) for t, m in ex.moves()]

        @pl.when(step == 0)
        def _():
            if n_move:
                ex.barrier()
                for sub in range(2):
                    ex.start(sub, 0)
            for a, b, (_, update) in zip(raw, done, params):
                _prepare(a, b, update)
        for g in range(1, steps):
            now = [m for d, m in due if d == g]
            if now:
                pl.when(step == g)(lambda now=now: [m() for m in now] and None)
        hand_in, hand_out = list(work_in), list(work_out)
        if own_in:
            slot = lax.rem(step, 2)

            def bring(g, i, spec, k):
                return pltpu.make_async_copy(_at(work_in[k], spec, grid, g), held[i].at[lax.rem(g, 2)], in_sem.at[lax.rem(g, 2), i])

            def take(g, i, spec, k):
                return pltpu.make_async_copy(held[len(own_in) + i].at[lax.rem(g, 2)], _at(work_out[k], spec, grid, g),
                                             out_sem.at[lax.rem(g, 2), i])

            @pl.when(step == 0)
            def _():
                for i, (k, spec) in enumerate(own_in):
                    bring(step, i, spec, k).start()

            @pl.when(step + 1 < steps)
            def _():
                for i, (k, spec) in enumerate(own_in):
                    bring(step + 1, i, spec, k).start()
            for i, (k, spec) in enumerate(own_in):
                bring(step, i, spec, k).wait()
                hand_in[k] = held[i].at[slot]

            @pl.when(step >= 2)
            def _():
                for i, (k, spec) in enumerate(own_out):
                    take(step - 2, i, spec, k).wait()
            for i, (k, spec) in enumerate(own_out):
                hand_out[k] = held[len(own_in) + i].at[slot]
        body(topo, *done, *hand_in, *hand_out, *work_scr)
        if own_in:
            for i, (k, spec) in enumerate(own_out):
                take(step, i, spec, k).start()

            @pl.when(step == steps - 1)
            def _():
                for g in range(max(0, steps - 2), steps):
                    for i, (k, spec) in enumerate(own_out):
                        take(g, i, spec, k).wait()
        if n_move:
            @pl.when(step == steps - 1)
            def _():
                for d, m in due:
                    if d >= steps:
                        m()
                ex.drain()

    return pl.pallas_call(kernel, grid=grid, out_shape=tuple(outs), in_specs=in_specs, out_specs=tuple(out_specs),
                          scratch_shapes=scratch + sems, compiler_params=pltpu.CompilerParams(**compiler), name=name)(*ins)


def project(sh, params, z, m, **move):
    return call(sh, "project", _project_kernel, sh.grid, params, (z, m), [sh.z_spec, sh.m_spec],
                [sh.sides], [sh.sides_spec], [sh.scr], **move)


def finish_project(sh, params, z, m, t, **move):
    return call(sh, "finish_project", _finish_project_kernel, sh.grid, params, (z, m, t[0]) + (t[1],) * sh.topo.nb,
                [sh.z_spec, sh.m_spec] + sh.tri_pieces(), [sh.zt, sh.sides], [sh.zt_spec, sh.sides_spec], [sh.scr_y, sh.scr], **move)


def finish(sh, params, zt, t, **move):
    return call(sh, "finish", _finish_kernel, sh.grid, params, (zt, t[0]) + (t[1],) * sh.topo.nb,
                [sh.zt_spec] + sh.tri_pieces(), [sh.z_out], [sh.z_spec], [sh.scr_y], **move)


def finish_last(sh, params, zt, t, other):
    return call(sh, "finish_last", _finish_last_kernel, sh.grid, params, (zt, other, t[0]) + (t[1],) * sh.topo.nb,
                [sh.zt_spec, sh.z_spec] + sh.tri_pieces(), [sh.z_out, sh.z_out], [sh.z_spec, sh.z_spec], [sh.scr_y])


def triangle(sh, sides, contract, **move):
    hbm = pl.BlockSpec(memory_space=pl.ANY)
    return call(sh, "triangle", lambda topo, *refs: _triangle_kernel(topo, contract, *refs), (sh.topo.nq,), (),
                sides, [hbm, hbm], [sh.tri], [hbm],
                [sh.mat, sh.mat, sh.mat, pltpu.SemaphoreType.DMA((2, 2)), pltpu.SemaphoreType.DMA((2,))], **move)


def solution(mesh):
    n = mesh.shape["dap"]
    row_spec = P(("data", "dap"), None, None)
    mask_spec = P(("data", "dap"), None)
    rep = P()

    def per_device(z_one, mask_one, z_two, mask_two, norm_in, w_proj, w_gate, norm_mid, w_out):
        sh = Shapes(n, z_one, w_proj)
        first = ((norm_in, 0), (w_proj, 0))
        middle = ((norm_in, 0), (norm_mid, 0), (w_gate, 0), (w_out, 0), (norm_in, 1), (w_proj, 1))
        last = ((norm_in, 1), (norm_mid, 1), (w_gate, 1), (w_out, 1))
        s1, = project(sh, first, z_one, mask_one)
        s2, w1 = project(sh, first, z_two, mask_two, moving=s1, cid=0, pace=6)
        t1, w2 = triangle(sh, (s1, w1), 1, moving=s2, cid=1)
        t2, v1 = triangle(sh, (s2, w2), 1, moving=t1, cid=2)
        zt1, s1, v2 = finish_project(sh, middle, z_one, mask_one, (t1, v1), moving=t2, cid=3, pace=1.3)
        zt2, s2, w1 = finish_project(sh, middle, z_two, mask_two, (t2, v2), moving=s1, cid=4, pace=3.2)
        t1, w2 = triangle(sh, (s1, w1), 0, moving=s2, cid=5)
        t2, v1 = triangle(sh, (s2, w2), 0, moving=t1, cid=6)
        z1, v2 = finish(sh, last, zt1, (t1, v1), moving=t2, cid=7, pace=3.4)
        z2, z1 = finish_last(sh, last, zt2, (t2, v2), z1)
        return z1, z2

    return jax.shard_map(per_device, mesh=mesh,
                         in_specs=(row_spec, mask_spec, row_spec, mask_spec, rep, rep, rep, rep, rep),
                         out_specs=(row_spec, row_spec), check_vma=False)
```
